32 devices in a mesh: dp: 4 (over y, x), expert: 8 (over z, core).
Axes of the slice: x: 2, y: 2, z: 4, core: 2. Of those that a mesh axis runs over, the one named last changes fastest.
Arguments:
- tokens: bfloat16 [8, 512, 4096], P('expert', 'dp'), may hold values from -6 to 6
- w_gate: bfloat16 [8, 4096, 896], P('expert'), may hold values from -0.09375 to 0.09375
- w_up: bfloat16 [8, 4096, 896], P('expert'), may hold values from -0.09375 to 0.09375
- w_down: bfloat16 [8, 896, 4096], P('expert'), may hold values from -0.1875 to 0.1875
- expert_ids: int32 [8, 512, 4], P('expert'), may hold values from 0 to 7, all different within a row
- gate_index: int32 [8, 512, 4], P('expert'), may hold values from 0 to 255
- gate_table: float32 [256], replicated, may hold values from 0.05 to 1
- spill: int32 [8, 512], P('expert'), may hold values from 0 to 3, as said below
Outputs:
- mixed: bfloat16 [8, 512, 4096], P('expert', 'dp')
The draws below stay inside these ranges and needn't reach their ends.
Inputs may be any that keep to these rules, and one draw needn't show every extreme that they name: `spill`: A token is dispatched by a device of its own column. Of the 128 tokens of one device at most 32 are dispatched by any one other device, and in every draw some device hands exactly 32 to some peer.
All inputs are finite; a program needn't handle non-finite values.
Results may differ from the reference program's by a relative error of at most 0.0058.
Values may be sent and summed in bfloat16 or wider, within the bound.
A program may use at most 128 MiB of HBM per device.

```python
import math
import jax
import jax.numpy as jnp
from jax import lax

D = 4096
FF = 896
TOP = 4
LEVELS = 256
TOK_DEV = 128
EXPERTS = 8
NCOL = 8
COL_TOK = 512
CAP = 96
SPILL = 32
N_DP = 4


def draw_spill(key, part):

    def column(column_key):
        count_key, perm_key, pick_key = jax.random.split(column_key, 3)
        counts = jax.random.randint(count_key, (N_DP, N_DP - 1), 0, SPILL + 1)
        full_home = jax.random.randint(pick_key, (), 0, N_DP)
        counts = counts.at[full_home, 0].set(SPILL)
        bounds = jnp.cumsum(counts, axis=1)
        positions = jax.vmap(lambda home_key: jax.random.permutation(home_key, TOK_DEV))(jax.random.split(perm_key, N_DP))
        passed = jnp.sum((positions[:, :, None] >= bounds[:, None, :]).astype(jnp.int32), axis=2)
        home_dev = jnp.arange(N_DP, dtype=jnp.int32)[:, None]
        senders = jnp.where(passed < N_DP - 1, (home_dev + 1 + passed) % N_DP, home_dev)
        return senders.reshape(-1).astype(jnp.int32)
    column_keys = jax.random.split(jax.random.fold_in(key, 17), NCOL)
    return jax.vmap(column)(column_keys)


def with_ends(result, stream_key, least, top_value):
    spot = [jax.random.randint(jax.random.fold_in(stream_key, axis), (), 0, length) for axis, length in enumerate(result.shape)]
    longest = result.shape.index(max(result.shape))
    next_to = spot[:longest] + [(spot[longest] + 1) % result.shape[longest]] + spot[longest + 1:]
    return result.at[tuple(spot)].set(least).at[tuple(next_to)].set(top_value)


def steps_of(stream_key, dims, pieces, low, largest):
    level = 1.0
    for position, parts in pieces:
        steps = jax.random.uniform(jax.random.fold_in(jax.random.fold_in(stream_key, 6), position), (parts,), jnp.float32, low / len(pieces), largest / len(pieces))
        level = level * jnp.repeat(jnp.exp(steps), dims[position] // parts).reshape((-1,) + (1,) * (len(dims) - 1 - position))
    return level


def different_ones(own_key, rows, number_of, top, lift):
    order = jax.random.permutation(jax.random.fold_in(own_key, 1), number_of)
    pull = order
    for power in range(3):
        pull = pull * pull // number_of
    pull = pull * lift // number_of
    chance = jax.random.randint(jax.random.fold_in(own_key, 2), (rows, number_of), 0, 4096) + pull
    fixed_rows = jax.random.permutation(jax.random.fold_in(own_key, 3), rows)[jnp.arange(number_of) % rows]
    chance = jnp.where(jnp.arange(rows)[:, None] == fixed_rows[None, :], 1 << 14, chance)
    priority = chance * number_of + jnp.arange(number_of)
    return lax.top_k(priority.astype(jnp.int32), top)[1].astype(jnp.int32)


def bell_draw(stream_key, shape, spread, bound, cuts=(), kind=jnp.bfloat16):
    values = jax.random.normal(stream_key, shape, jnp.float32) * spread
    if len(cuts) > 0:
        values = steps_of(stream_key, shape, cuts, -0.22, 0.18) * values
    return jnp.clip(values, min=-bound, max=bound).astype(kind)


def setup_inputs(seed: int = 0) -> dict:
    seeds = jax.random.split(jax.random.key(seed), 9)
    tokens = bell_draw(seeds[0], (NCOL, COL_TOK, D), 1.0, 6.0, ((0, 8), (1, 4)))
    w_gate = bell_draw(seeds[1], (EXPERTS, D, FF), D ** -0.5, 0.09375, ((0, 8),))
    w_up = bell_draw(seeds[2], (EXPERTS, D, FF), D ** -0.5, 0.09375, ((0, 8),))
    w_down = bell_draw(seeds[3], (EXPERTS, FF, D), FF ** -0.5, 0.1875, ((0, 8),))
    expert_ids = different_ones(seeds[4], NCOL * COL_TOK, EXPERTS, TOP, 8192).reshape((NCOL, COL_TOK, TOP))
    gate_index = with_ends(jax.random.randint(seeds[5], (NCOL, COL_TOK, TOP), 0, LEVELS), jax.random.fold_in(seeds[5], 1), 0, LEVELS - 1).astype(jnp.int32)
    gate_table = jnp.clip(jnp.exp(jax.random.uniform(seeds[6], (LEVELS,), jnp.float32, math.log(0.05), math.log(1.0))), 0.05, 1.0)
    spill = draw_spill(jax.random.fold_in(seeds[8], 71), 0)
    return dict(tokens=tokens, w_gate=w_gate, w_up=w_up, w_down=w_down, expert_ids=expert_ids, gate_index=gate_index, gate_table=gate_table, spill=spill)


def rank_within(route_row, key_count):
    onehot = (route_row[:, None] == jnp.arange(key_count, dtype=jnp.int32)[None, :]).astype(jnp.int32)
    return jnp.sum((jnp.cumsum(onehot, axis=0) - onehot) * onehot, axis=1).astype(jnp.int32)


def reference(tokens, w_gate, w_up, w_down, expert_ids, gate_index, gate_table, spill):
    ncol_count = tokens.shape[0]
    column_tokens = tokens.shape[1]
    model_width = tokens.shape[2]
    experts_all = w_gate.shape[0]
    top_count = expert_ids.shape[2]
    picked = gate_table[gate_index]
    weight = picked / jnp.sum(picked, axis=-1, keepdims=True)
    pair_sender = jnp.repeat(spill, top_count, axis=1).astype(jnp.int32)
    flat_ids = expert_ids.reshape(ncol_count, column_tokens * top_count).astype(jnp.int32)
    route_key = pair_sender * experts_all + flat_ids
    slot_rank = lax.map(lambda row: rank_within(row, N_DP * experts_all), route_key)
    is_kept = slot_rank < CAP
    per_expert = ncol_count * N_DP * CAP
    column_base = jnp.arange(ncol_count, dtype=jnp.int32)[:, None]
    slot_index = (column_base * N_DP + pair_sender) * CAP + slot_rank
    slot_index = jnp.where(is_kept, slot_index, per_expert).astype(jnp.int32)
    token_total = ncol_count * column_tokens
    pair_token = column_base * column_tokens + jnp.arange(column_tokens * top_count, dtype=jnp.int32)[None, :] // top_count
    row_source = jnp.full((experts_all, per_expert + 1), token_total, jnp.int32)
    row_source = row_source.at[flat_ids, slot_index].set(pair_token.astype(jnp.int32))[:, :per_expert]
    kept_weight = jnp.where(is_kept, weight.reshape(ncol_count, column_tokens * top_count), 0.0).astype(jnp.float32)
    row_scale = jnp.zeros((experts_all, per_expert + 1), jnp.float32)
    row_scale = row_scale.at[flat_ids, slot_index].set(kept_weight)[:, :per_expert]
    padded = jnp.concatenate([tokens.reshape(token_total, model_width), jnp.zeros((1, model_width), tokens.dtype)], axis=0)

    def expert_step(totals, inputs):
        gate_mat, up_mat, down_mat, sources, scales = inputs
        rows_in = padded[sources]
        gate_part = jnp.dot(rows_in, gate_mat, preferred_element_type=jnp.float32)
        up_part = jnp.dot(rows_in, up_mat, preferred_element_type=jnp.float32)
        hidden = (jax.nn.silu(gate_part) * up_part).astype(jnp.bfloat16)
        expert_out = jnp.dot(hidden, down_mat, preferred_element_type=jnp.float32).astype(jnp.bfloat16)
        totals = totals.at[sources].add(scales[:, None] * expert_out.astype(jnp.float32))
        return totals, None

    start = jnp.zeros((token_total + 1, model_width), jnp.float32)
    totals, unused = lax.scan(expert_step, start, (w_gate, w_up, w_down, row_source, row_scale))
    return totals[:token_total].astype(jnp.bfloat16).reshape(ncol_count, column_tokens, model_width)
```

```python
import functools
import jax
import jax.numpy as jnp
from jax import lax
from jax.experimental import pallas as pl
from jax.experimental.pallas import tpu as pltpu
from jax.sharding import PartitionSpec as P


def exchange_plan(tokens, w_gate, w_up, w_down, expert_ids, gate_index, gate_table, spill):
    dp_count = lax.axis_size("dp")
    expert_count = lax.axis_size("expert")
    local_experts = w_gate.shape[0]
    experts_all = local_experts * expert_count
    own_rows = tokens.shape[1]
    model_width = tokens.shape[2]
    column_tokens = spill.shape[1]
    top_count = expert_ids.shape[2]
    capacity = 3 * own_rows * top_count // (2 * experts_all)
    spill_room = own_rows // 4
    dp_index = lax.axis_index("dp")
    senders = spill[0]
    flat_ids = expert_ids[0].reshape(-1)
    level_count = gate_table.shape[0]
    matches = gate_index[0][:, :, None] == jnp.arange(level_count, dtype=jnp.int32)
    picked = jnp.sum(jnp.where(matches, gate_table, 0.0), axis=2)
    weight = picked / jnp.sum(picked, axis=1, keepdims=True)
    pair_sender = jnp.repeat(senders, top_count)
    is_mine = pair_sender == dp_index
    onehot = (
        (flat_ids[:, None] == jnp.arange(experts_all, dtype=jnp.int32)) & is_mine[:, None]
    ).astype(jnp.int32)
    slot_rank = jnp.sum((jnp.cumsum(onehot, axis=0) - onehot) * onehot, axis=1)
    is_kept = is_mine & (slot_rank < capacity)
    empty_slot = experts_all * capacity
    slot_index = jnp.where(is_kept, flat_ids * capacity + slot_rank, empty_slot)
    pair_token = jnp.arange(column_tokens * top_count, dtype=jnp.int32) // top_count
    zero_row = jnp.zeros((1, model_width), tokens.dtype)
    token_ids = jnp.arange(column_tokens, dtype=jnp.int32)
    home_dev = token_ids // own_rows
    local_token = token_ids - home_dev * own_rows
    is_moved = senders != home_dev
    route_key = home_dev * dp_count + senders
    route_hot = (route_key[:, None] == jnp.arange(dp_count * dp_count, dtype=jnp.int32)).astype(
        jnp.int32
    )
    spill_rank = jnp.sum((jnp.cumsum(route_hot, axis=0) - route_hot) * route_hot, axis=1)
    incoming = is_moved & (senders == dp_index)
    spill_slots = dp_count * spill_room
    outgoing = is_moved & (home_dev == dp_index)
    send_target = jnp.where(outgoing, senders * spill_room + spill_rank, spill_slots)
    send_source = (
        jnp.full((spill_slots,), own_rows, jnp.int32).at[send_target].set(local_token, mode="drop")
    )
    own_padded = jnp.concatenate([tokens[0], zero_row], axis=0)
    outgoing_rows = own_padded[send_source].reshape(dp_count, spill_room, model_width)
    arrived = lax.all_to_all(outgoing_rows, "dp", split_axis=0, concat_axis=0, tiled=True)
    source_rows = jnp.concatenate(
        [tokens[0], arrived.reshape(spill_slots, model_width), zero_row], axis=0
    )
    token_row = jnp.where(
        home_dev == dp_index,
        local_token,
        jnp.where(incoming, own_rows + home_dev * spill_room + spill_rank, own_rows + spill_slots),
    )
    dispatch_source = (
        jnp.full((empty_slot,), source_rows.shape[0] - 1, jnp.int32)
        .at[slot_index]
        .set(token_row[pair_token], mode="drop")
    )
    outbound = source_rows[dispatch_source].reshape(
        expert_count, local_experts, capacity, model_width
    )
    block = lax.all_to_all(outbound, "expert", split_axis=0, concat_axis=0, tiled=True)
    gate_part = jnp.einsum("aecd,edf->aecf", block, w_gate, preferred_element_type=jnp.float32)
    up_part = jnp.einsum("aecd,edf->aecf", block, w_up, preferred_element_type=jnp.float32)
    hidden = (jax.nn.silu(gate_part) * up_part).astype(jnp.bfloat16)
    expert_out = jnp.einsum(
        "aecf,efd->aecd", hidden, w_down, preferred_element_type=jnp.float32
    ).astype(jnp.bfloat16)
    returned = lax.all_to_all(expert_out, "expert", split_axis=0, concat_axis=0, tiled=True)
    results = jnp.concatenate([returned.reshape(empty_slot, model_width), zero_row], axis=0)
    slot_grid = jnp.concatenate(
        [
            slot_index.reshape(column_tokens, top_count),
            jnp.full((1, top_count), empty_slot, jnp.int32),
        ],
        axis=0,
    )
    kept_scale = jnp.where(is_kept.reshape(column_tokens, top_count), weight, 0.0)
    scale_grid = jnp.concatenate([kept_scale, jnp.zeros((1, top_count), jnp.float32)], axis=0)

    def combine(chosen):
        chosen_slots = slot_grid[chosen]
        chosen_scale = scale_grid[chosen]
        summed = jnp.zeros((chosen.shape[0], model_width), jnp.float32)
        for member in range(top_count):
            summed = summed + chosen_scale[:, member : member + 1] * results[
                chosen_slots[:, member]
            ].astype(jnp.float32)
        return summed

    own_ids = dp_index * own_rows + jnp.arange(own_rows, dtype=jnp.int32)
    own_part = combine(own_ids)
    arrived_target = jnp.where(incoming, home_dev * spill_room + spill_rank, spill_slots)
    arrived_ids = (
        jnp.full((spill_slots,), column_tokens, jnp.int32)
        .at[arrived_target]
        .set(token_ids, mode="drop")
    )
    arrived_part = combine(arrived_ids).reshape(dp_count, spill_room, model_width)
    returned_part = lax.all_to_all(
        arrived_part.astype(jnp.bfloat16), "dp", split_axis=0, concat_axis=0, tiled=True
    ).astype(arrived_part.dtype)
    back_rows = jnp.concatenate(
        [returned_part.reshape(spill_slots, model_width), jnp.zeros((1, model_width), jnp.float32)],
        axis=0,
    )
    back_pick = jnp.where(
        is_moved[own_ids], senders[own_ids] * spill_room + spill_rank[own_ids], spill_slots
    )
    mixed = own_part + back_rows[back_pick]
    return mixed.astype(jnp.bfloat16)[None]


CORES = 2
HALVES = 2
PIECES = 4
LEAD = 2
IN_TILES = 2
MESH = pl.DeviceIdType.MESH


def token_scales(expert_ids, gate_index, gate_table, spill, own_rows, experts_all):
    top_count, column_tokens = expert_ids.shape[1:]
    capacity = 3 * own_rows * top_count // (2 * experts_all)
    first = pl.multiple_of(lax.axis_index("dp") * own_rows, own_rows)
    own = pl.ds(first, own_rows)
    experts = lax.broadcasted_iota(jnp.int32, (experts_all, column_tokens), 0)
    chosen = jnp.zeros((experts_all, column_tokens), jnp.float32)
    for k in range(top_count):
        chosen += jnp.where(expert_ids[0, k : k + 1, :] == experts, 1.0, 0.0)
    own_row = spill[:, own].astype(jnp.float32)
    own_senders = jnp.transpose(jnp.broadcast_to(own_row, (own_rows, own_rows)))[:, :1]
    shape = (own_rows, column_tokens)
    before = lax.broadcasted_iota(jnp.int32, shape, 1) < first + lax.broadcasted_iota(
        jnp.int32, shape, 0
    )
    earlier = before & (spill[...].astype(jnp.float32) == own_senders)
    rank = lax.dot_general(
        chosen.astype(jnp.bfloat16),
        jnp.where(earlier, 1.0, 0.0).astype(jnp.bfloat16),
        (((1,), (1,)), ((), ())),
        preferred_element_type=jnp.float32,
    )
    level_count = gate_table.shape[1]
    levels = lax.broadcasted_iota(jnp.int32, (level_count, own_rows), 0)
    table = jnp.transpose(jnp.broadcast_to(gate_table[...], (own_rows, level_count)))
    picked = [
        jnp.sum(
            jnp.where(gate_index[0, k : k + 1, own] == levels, table, 0.0), axis=0, keepdims=True
        )
        for k in range(top_count)
    ]
    norm = functools.reduce(jnp.add, picked)
    own_experts = lax.broadcasted_iota(jnp.int32, (experts_all, own_rows), 0)
    scale = jnp.zeros((experts_all, own_rows), jnp.float32)
    for k in range(top_count):
        scale += jnp.where(expert_ids[0, k : k + 1, own] == own_experts, picked[k] / norm, 0.0)
    return jnp.where(rank < capacity, scale, 0.0)


def line_kernel(
    chips, tok, w_gate, w_up, w_down, expert_ids, gate_index, gate_table, spill, out,
    x, w_in, w_out, scales, cols_of, both, hid, part, near, from_left, from_right, going, total,
    own_sem, sc_right, sc_left, sc_sib, sc_r, sc_sib_r,
    ag_right, ag_left, ag_sib, ag_r, sib_r, part_s, part_r, go_s, left_r, right_r,
):
    own_rows, width = tok.shape[1], tok.shape[2]
    hidden_units = w_gate.shape[2]
    half = own_rows // HALVES
    piece = half // PIECES
    tile = width // PIECES
    count = chips * CORES
    slots = 2 * chips
    me = lax.axis_index("expert")
    p = me // CORES
    q = lax.rem(me, CORES)
    sib = p * CORES + 1 - q
    right, left = me + CORES, me - CORES
    has_right, has_left = p < chips - 1, p > 0

    def send(src, dst, send_sem, recv_sem, device):
        return pltpu.make_async_remote_copy(
            src_ref=src, dst_ref=dst, send_sem=send_sem, recv_sem=recv_sem,
            device_id={"expert": device}, device_id_type=MESH,
        )

    def gather_copy(s, c, send_sem, recv_sem, device):
        block = x.at[CORES * s + q, pl.ds(pl.multiple_of(c * piece, piece), piece)]
        return send(block, block, send_sem.at[s], recv_sem.at[s, c], device)

    def scale_copy(s, send_sem, recv_sem, device):
        block = scales.at[CORES * s + q]
        return send(block, block, send_sem.at[s], recv_sem.at[s], device)

    sides = (
        (p, has_right, right, ag_right, sc_right, from_left, left_r),
        (chips - 1 - p, has_left, left, ag_left, sc_left, from_right, right_r),
    )

    loads = [
        pltpu.make_async_copy(tok.at[0], x.at[me], own_sem.at[0]),
        pltpu.make_async_copy(w_gate.at[0], w_in.at[:, pl.ds(0, hidden_units)], own_sem.at[1]),
        pltpu.make_async_copy(w_up.at[0], w_in.at[:, pl.ds(hidden_units, hidden_units)], own_sem.at[2]),
        pltpu.make_async_copy(w_down.at[0], w_out, own_sem.at[3]),
    ]
    for load in loads:
        load.start()
    barrier = pltpu.get_barrier_semaphore()

    def greet(device):
        pl.semaphore_signal(barrier, inc=1, device_id={"expert": device}, device_id_type=MESH)

    greet(sib)
    pl.when(has_right)(lambda: greet(right))
    pl.when(has_left)(lambda: greet(left))
    pl.semaphore_wait(barrier, 1 + has_right.astype(jnp.int32) + has_left.astype(jnp.int32))
    loads[0].wait()

    def first_sends(c, carry):
        for _, there, device, ag, *_ in sides:
            pl.when(there)(lambda: gather_copy(p, c, ag, ag_r, device).start())
        return carry

    def sib_sends(c, carry):
        gather_copy(p, c, ag_sib, sib_r, sib).start()
        return carry

    lax.fori_loop(0, PIECES, first_sends, 0)
    lax.fori_loop(0, HALVES * PIECES, sib_sends, 0)
    scales[me] = token_scales(expert_ids, gate_index, gate_table, spill, own_rows, count)
    for _, there, device, _, sc, *_ in sides:
        pl.when(there)(lambda: scale_copy(p, sc, sc_r, device).start())
    scale_copy(p, sc_sib, sc_sib_r, sib).start()

    tall = CORES * half
    in_tile = 2 * hidden_units // IN_TILES

    def block_rows(h):
        return pl.ds(pl.multiple_of(h * half, half), half)

    def enter(s, h):
        @pl.when((s == p) & (h == 0))
        def _():
            loads[1].wait()
            loads[2].wait()

        def arrived(t, carry):
            block = x.at[CORES * s + 1 - q, pl.ds(pl.multiple_of((h * PIECES + t) * piece, piece), piece)]
            send(block, block, ag_sib.at[s], sib_r.at[s, h * PIECES + t], sib).wait_recv()
            return carry

        lax.fori_loop(0, PIECES, arrived, 0)

        def one(t, carry):
            cols = pl.ds(pl.multiple_of(t * in_tile, 128), in_tile)
            tokens = x[pl.ds(CORES * s, CORES), block_rows(h)].reshape(tall, width)
            both[:, cols] = jnp.dot(tokens, w_in[:, cols], preferred_element_type=jnp.float32)
            return carry

        lax.fori_loop(0, IN_TILES, one, 0)

    def near_copy(s, h, t):
        return send(
            part.at[CORES * s + 1 - q, h, t], near.at[s, h, t],
            part_s.at[s], part_r.at[s, h * PIECES + t], sib,
        )

    def leave(s, h):
        @pl.when((s == p) & (h == 0))
        def _():
            loads[3].wait()

        @pl.when(h == 0)
        def _():
            block = scales.at[CORES * s + 1 - q]
            send(block, block, sc_sib.at[s], sc_sib_r.at[s], sib).wait_recv()
            for core in range(CORES):
                row = scales[CORES * s + core, pl.ds(me, 1), :]
                cols_of[s, core] = jnp.transpose(jnp.broadcast_to(row, (own_rows, own_rows)))

        for core in range(CORES):
            part_rows = pl.ds(core * half, half)
            col = cols_of[s, core, block_rows(h), :][:, :1]
            gate = both[part_rows, pl.ds(0, hidden_units)]
            up = both[part_rows, pl.ds(hidden_units, hidden_units)]
            hid[part_rows, :] = (gate / (1.0 + jnp.exp(-gate)) * up * col).astype(hid.dtype)

        def one(t, carry):
            cols = pl.ds(pl.multiple_of(t * tile, 128), tile)
            made = jnp.dot(hid[...], w_out[:, cols], preferred_element_type=jnp.float32)
            part[pl.ds(CORES * s, CORES), h, t] = made.astype(part.dtype).reshape(CORES, half, tile)
            near_copy(s, h, t).start()
            return carry

        lax.fori_loop(0, PIECES, one, 0)

    def pair_sum(s, h, t):
        return part[CORES * s + q, h, t].astype(jnp.float32) + near[s, h, t].astype(jnp.float32)

    def came_wait(came, came_sem, s, h, t):
        block = came.at[s, h, t]
        send(block, block, go_s.at[s], came_sem.at[s, h * PIECES + t], sib).wait_recv()

    def gathers(at, side, place, there, device, ag, sc, came, came_sem):
        k, t = at // PIECES, lax.rem(at, PIECES)
        h = (k > place).astype(jnp.int32)
        origin = jnp.where(k > place, k - place - 1, place - k)
        s = origin if side == 0 else chips - 1 - origin
        active = (k > 0) & (k <= 2 * place + 1)
        c = h * PIECES + t

        @pl.when(active & (s != p))
        def _():
            gather_copy(s, c, ag, ag_r, sib).wait_recv()
            gather_copy(s, c, ag_sib, sib_r, sib).start()

            @pl.when(c == 0)
            def _():
                scale_copy(s, sc, sc_r, sib).wait_recv()
                scale_copy(s, sc_sib, sc_sib_r, sib).start()
                pl.when(there)(lambda: scale_copy(s, sc, sc_r, device).start())

        pl.when(active & there)(lambda: gather_copy(s, c, ag, ag_r, device).start())

    def sums(at, side, place, there, device, ag, sc, came, came_sem):
        k, t = at // PIECES, lax.rem(at, PIECES)
        i = k - (2 * place + 2)
        n = chips - 1 - place
        h = (i >= n).astype(jnp.int32)
        target = place + 1 + jnp.where(i >= n, 2 * n - 1 - i, i)
        s = target if side == 0 else chips - 1 - target

        @pl.when((i >= 0) & (k < slots))
        def _():
            near_copy(s, h, t).wait_recv()

            @pl.when(place == 0)
            def _():
                going[s, h, t] = pair_sum(s, h, t).astype(going.dtype)

            @pl.when(place > 0)
            def _():
                came_wait(came, came_sem, s, h, t)
                summed = pair_sum(s, h, t) + came[s, h, t].astype(jnp.float32)
                going[s, h, t] = summed.astype(going.dtype)

            send(
                going.at[s, h, t], came.at[s, h, t],
                go_s.at[s], came_sem.at[s, h * PIECES + t], device,
            ).start()

    def unit(k, second):
        mirror = (p >= chips - p) == second
        place = jnp.where(mirror, chips - 1 - p, p)
        origin = jnp.where(k > place, k - place - 1, place - k)
        own = k == 0
        s = jnp.where(own, p, jnp.where(mirror, chips - 1 - origin, origin))
        h = jnp.where(own, second.astype(jnp.int32), (k > place).astype(jnp.int32))
        return own | (k <= 2 * place), s, h

    def period(m, carry):
        at = m + LEAD
        for side, args in enumerate(sides):
            @pl.when(at < slots * PIECES)
            def _():
                gathers(at, side, *args)

        since = m - 1
        k, phase = since // 4, lax.rem(since, 4)
        active, s, h = unit(k, phase >= 2)
        active &= (since >= 0) & (k < slots - 1)
        pl.when(active & (lax.rem(phase, 2) == 0))(lambda: enter(s, h))
        pl.when(active & (lax.rem(phase, 2) == 1))(lambda: leave(s, h))
        for side, args in enumerate(sides):
            sums(at, side, *args)

        last = m - ((slots - HALVES) * PIECES + LEAD)
        h_last, t_last = last // PIECES, lax.rem(last, PIECES)

        @pl.when(last >= 0)
        def _():
            near_copy(p, h_last, t_last).wait_recv()
            total[...] = pair_sum(p, h_last, t_last)
            for there, came, came_sem in (
                (has_left, from_left, left_r), (has_right, from_right, right_r)
            ):
                @pl.when(there)
                def _():
                    came_wait(came, came_sem, p, h_last, t_last)
                    total[...] += came[p, h_last, t_last].astype(jnp.float32)

            cols = pl.ds(pl.multiple_of(t_last * tile, 128), tile)
            out[0, block_rows(h_last), cols] = total[...].astype(out.dtype)

        return carry

    lax.fori_loop(0, slots * PIECES + LEAD, period, 0)

    def drain(s, carry):
        mine = x.at[CORES * s + q]
        send(mine, mine, ag_sib.at[s], ag_r.at[s, 0], sib).wait_send()
        scale_copy(s, sc_sib, sc_sib_r, sib).wait_send()
        for there, ahead, ag, sc in ((has_right, s <= p, ag_right, sc_right), (has_left, s >= p, ag_left, sc_left)):
            @pl.when(there & ahead)
            def _():
                send(mine, mine, ag.at[s], ag_r.at[s, 0], sib).wait_send()
                scale_copy(s, sc, sc_r, sib).wait_send()

        given = part.at[CORES * s + 1 - q]
        send(given, given, part_s.at[s], ag_r.at[s, 0], sib).wait_send()

        @pl.when(s != p)
        def _():
            block = going.at[s]
            send(block, block, go_s.at[s], ag_r.at[s, 0], sib).wait_send()

        return carry

    lax.fori_loop(0, chips, drain, 0)


def scratch_of(chips, own_rows, width, hidden_units, experts_all, dtype):
    count = chips * CORES
    half = own_rows // HALVES
    tile = width // PIECES
    tiles = (HALVES, PIECES, half, tile)
    sums = pltpu.VMEM((chips, *tiles), dtype)
    dma = pltpu.SemaphoreType.DMA
    line = dma((chips,))
    pieces = dma((chips, HALVES * PIECES))
    return [
        pltpu.VMEM((count, own_rows, width), dtype),
        pltpu.VMEM((width, 2 * hidden_units), dtype),
        pltpu.VMEM((hidden_units, width), dtype),
        pltpu.VMEM((count, experts_all, own_rows), jnp.float32),
        pltpu.VMEM((chips, CORES, own_rows, own_rows), jnp.float32),
        pltpu.VMEM((CORES * half, 2 * hidden_units), jnp.float32),
        pltpu.VMEM((CORES * half, hidden_units), dtype),
        pltpu.VMEM((count, *tiles), dtype),
        sums, sums, sums, sums,
        pltpu.VMEM((half, tile), jnp.float32),
        dma((4,)),
        line, line, line, line, line,
        line, line, line, pieces, pieces, line, pieces, line, pieces, pieces,
    ]


def line_plan(tokens, w_gate, w_up, w_down, expert_ids, gate_index, gate_table, spill):
    experts_all = lax.axis_size("expert")
    own_rows, width = tokens.shape[1:]
    chips = experts_all // CORES
    anywhere = pl.BlockSpec(memory_space=pl.ANY)
    vmem = pl.BlockSpec(memory_space=pltpu.VMEM)
    return pl.pallas_call(
        functools.partial(line_kernel, chips),
        out_shape=jax.ShapeDtypeStruct(tokens.shape, tokens.dtype),
        in_specs=[anywhere] * 4 + [vmem] * 4,
        out_specs=vmem,
        scratch_shapes=scratch_of(
            chips, own_rows, width, w_gate.shape[2], experts_all, tokens.dtype
        ),
        compiler_params=pltpu.CompilerParams(
            collective_id=0, has_side_effects=True, vmem_limit_bytes=67043328
        ),
    )(
        tokens, w_gate, w_up, w_down,
        jnp.swapaxes(expert_ids, 1, 2), jnp.swapaxes(gate_index, 1, 2), gate_table[None], spill,
    )


def local(tokens, w_gate, w_up, w_down, *routing):
    own_rows, width = tokens.shape[1:]
    experts_all = lax.axis_size("expert")
    held = w_gate.size + w_up.size + w_down.size + 4 * experts_all * own_rows * width
    fits = held * tokens.dtype.itemsize <= 56 * 2**20
    cut = own_rows % (HALVES * PIECES * 16) == 0 and width % (PIECES * 128) == 0
    line = w_gate.shape[0] == 1 and experts_all % CORES == 0 and experts_all > CORES
    if fits and cut and line:
        return line_plan(tokens, w_gate, w_up, w_down, *routing)
    return exchange_plan(tokens, w_gate, w_up, w_down, *routing)


def solution(mesh):
    in_specs = (
        P("expert", "dp", None),
        P("expert", None, None),
        P("expert", None, None),
        P("expert", None, None),
        P("expert", None, None),
        P("expert", None, None),
        P(),
        P("expert", None),
    )
    out_specs = P("expert", "dp", None)
    return jax.shard_map(local, mesh=mesh, in_specs=in_specs, out_specs=out_specs, check_vma=False)
```

```python
import functools
import jax
import jax.numpy as jnp
from jax import lax
from jax.experimental import pallas as pl
from jax.experimental.pallas import tpu as pltpu
from jax.sharding import PartitionSpec as P


def exchange_plan(tokens, w_gate, w_up, w_down, expert_ids, gate_index, gate_table, spill):
    dp_count = lax.axis_size("dp")
    expert_count = lax.axis_size("expert")
    local_experts = w_gate.shape[0]
    experts_all = local_experts * expert_count
    own_rows = tokens.shape[1]
    model_width = tokens.shape[2]
    column_tokens = spill.shape[1]
    top_count = expert_ids.shape[2]
    capacity = 3 * own_rows * top_count // (2 * experts_all)
    spill_room = own_rows // 4
    dp_index = lax.axis_index("dp")
    senders = spill[0]
    flat_ids = expert_ids[0].reshape(-1)
    level_count = gate_table.shape[0]
    matches = gate_index[0][:, :, None] == jnp.arange(level_count, dtype=jnp.int32)
    picked = jnp.sum(jnp.where(matches, gate_table, 0.0), axis=2)
    weight = picked / jnp.sum(picked, axis=1, keepdims=True)
    pair_sender = jnp.repeat(senders, top_count)
    is_mine = pair_sender == dp_index
    onehot = (
        (flat_ids[:, None] == jnp.arange(experts_all, dtype=jnp.int32)) & is_mine[:, None]
    ).astype(jnp.int32)
    slot_rank = jnp.sum((jnp.cumsum(onehot, axis=0) - onehot) * onehot, axis=1)
    is_kept = is_mine & (slot_rank < capacity)
    empty_slot = experts_all * capacity
    slot_index = jnp.where(is_kept, flat_ids * capacity + slot_rank, empty_slot)
    pair_token = jnp.arange(column_tokens * top_count, dtype=jnp.int32) // top_count
    zero_row = jnp.zeros((1, model_width), tokens.dtype)
    token_ids = jnp.arange(column_tokens, dtype=jnp.int32)
    home_dev = token_ids // own_rows
    local_token = token_ids - home_dev * own_rows
    is_moved = senders != home_dev
    route_key = home_dev * dp_count + senders
    route_hot = (route_key[:, None] == jnp.arange(dp_count * dp_count, dtype=jnp.int32)).astype(
        jnp.int32
    )
    spill_rank = jnp.sum((jnp.cumsum(route_hot, axis=0) - route_hot) * route_hot, axis=1)
    incoming = is_moved & (senders == dp_index)
    spill_slots = dp_count * spill_room
    outgoing = is_moved & (home_dev == dp_index)
    send_target = jnp.where(outgoing, senders * spill_room + spill_rank, spill_slots)
    send_source = (
        jnp.full((spill_slots,), own_rows, jnp.int32).at[send_target].set(local_token, mode="drop")
    )
    own_padded = jnp.concatenate([tokens[0], zero_row], axis=0)
    outgoing_rows = own_padded[send_source].reshape(dp_count, spill_room, model_width)
    arrived = lax.all_to_all(outgoing_rows, "dp", split_axis=0, concat_axis=0, tiled=True)
    source_rows = jnp.concatenate(
        [tokens[0], arrived.reshape(spill_slots, model_width), zero_row], axis=0
    )
    token_row = jnp.where(
        home_dev == dp_index,
        local_token,
        jnp.where(incoming, own_rows + home_dev * spill_room + spill_rank, own_rows + spill_slots),
    )
    dispatch_source = (
        jnp.full((empty_slot,), source_rows.shape[0] - 1, jnp.int32)
        .at[slot_index]
        .set(token_row[pair_token], mode="drop")
    )
    outbound = source_rows[dispatch_source].reshape(
        expert_count, local_experts, capacity, model_width
    )
    block = lax.all_to_all(outbound, "expert", split_axis=0, concat_axis=0, tiled=True)
    gate_part = jnp.einsum("aecd,edf->aecf", block, w_gate, preferred_element_type=jnp.float32)
    up_part = jnp.einsum("aecd,edf->aecf", block, w_up, preferred_element_type=jnp.float32)
    hidden = (jax.nn.silu(gate_part) * up_part).astype(jnp.bfloat16)
    expert_out = jnp.einsum(
        "aecf,efd->aecd", hidden, w_down, preferred_element_type=jnp.float32
    ).astype(jnp.bfloat16)
    returned = lax.all_to_all(expert_out, "expert", split_axis=0, concat_axis=0, tiled=True)
    results = jnp.concatenate([returned.reshape(empty_slot, model_width), zero_row], axis=0)
    slot_grid = jnp.concatenate(
        [
            slot_index.reshape(column_tokens, top_count),
            jnp.full((1, top_count), empty_slot, jnp.int32),
        ],
        axis=0,
    )
    kept_scale = jnp.where(is_kept.reshape(column_tokens, top_count), weight, 0.0)
    scale_grid = jnp.concatenate([kept_scale, jnp.zeros((1, top_count), jnp.float32)], axis=0)

    def combine(chosen):
        chosen_slots = slot_grid[chosen]
        chosen_scale = scale_grid[chosen]
        summed = jnp.zeros((chosen.shape[0], model_width), jnp.float32)
        for member in range(top_count):
            summed = summed + chosen_scale[:, member : member + 1] * results[
                chosen_slots[:, member]
            ].astype(jnp.float32)
        return summed

    own_ids = dp_index * own_rows + jnp.arange(own_rows, dtype=jnp.int32)
    own_part = combine(own_ids)
    arrived_target = jnp.where(incoming, home_dev * spill_room + spill_rank, spill_slots)
    arrived_ids = (
        jnp.full((spill_slots,), column_tokens, jnp.int32)
        .at[arrived_target]
        .set(token_ids, mode="drop")
    )
    arrived_part = combine(arrived_ids).reshape(dp_count, spill_room, model_width)
    returned_part = lax.all_to_all(
        arrived_part.astype(jnp.bfloat16), "dp", split_axis=0, concat_axis=0, tiled=True
    ).astype(arrived_part.dtype)
    back_rows = jnp.concatenate(
        [returned_part.reshape(spill_slots, model_width), jnp.zeros((1, model_width), jnp.float32)],
        axis=0,
    )
    back_pick = jnp.where(
        is_moved[own_ids], senders[own_ids] * spill_room + spill_rank[own_ids], spill_slots
    )
    mixed = own_part + back_rows[back_pick]
    return mixed.astype(jnp.bfloat16)[None]


CORES = 2
HALVES = 2
PIECES = 4
LEAD = PIECES // 2
IN_TILES = 1
OUT_TILES = 2
MESH = pl.DeviceIdType.MESH


def token_scales(expert_ids, gate_index, gate_table, spill, own_rows, experts_all):
    top_count, column_tokens = expert_ids.shape[1:]
    capacity = 3 * own_rows * top_count // (2 * experts_all)
    first = pl.multiple_of(lax.axis_index("dp") * own_rows, own_rows)
    own = pl.ds(first, own_rows)
    experts = lax.broadcasted_iota(jnp.int32, (experts_all, column_tokens), 0)
    chosen = jnp.zeros((experts_all, column_tokens), jnp.float32)
    for k in range(top_count):
        chosen += jnp.where(expert_ids[0, k : k + 1, :] == experts, 1.0, 0.0)
    own_row = spill[:, own].astype(jnp.float32)
    own_senders = jnp.transpose(jnp.broadcast_to(own_row, (own_rows, own_rows)))[:, :1]
    shape = (own_rows, column_tokens)
    before = lax.broadcasted_iota(jnp.int32, shape, 1) < first + lax.broadcasted_iota(
        jnp.int32, shape, 0
    )
    earlier = before & (spill[...].astype(jnp.float32) == own_senders)
    rank = lax.dot_general(
        chosen.astype(jnp.bfloat16),
        jnp.where(earlier, 1.0, 0.0).astype(jnp.bfloat16),
        (((1,), (1,)), ((), ())),
        preferred_element_type=jnp.float32,
    )
    level_count = gate_table.shape[1]
    levels = lax.broadcasted_iota(jnp.int32, (level_count, own_rows), 0)
    table = jnp.transpose(jnp.broadcast_to(gate_table[...], (own_rows, level_count)))
    picked = [
        jnp.sum(
            jnp.where(gate_index[0, k : k + 1, own] == levels, table, 0.0), axis=0, keepdims=True
        )
        for k in range(top_count)
    ]
    norm = functools.reduce(jnp.add, picked)
    own_experts = lax.broadcasted_iota(jnp.int32, (experts_all, own_rows), 0)
    scale = jnp.zeros((experts_all, own_rows), jnp.float32)
    for k in range(top_count):
        scale += jnp.where(expert_ids[0, k : k + 1, own] == own_experts, picked[k] / norm, 0.0)
    return jnp.where(rank < capacity, scale, 0.0)


def line_kernel(
    chips, tok, w_gate, w_up, w_down, ids_in, index_in, table_in, spill_in, out,
    expert_ids, gate_index, gate_table, spill, x, w_in, w_out, scales, cols_of, both, hid, part, near, from_left, from_right, going, total,
    tok_sem, own_sem, sc_right, sc_left, sc_sib, sc_r, sc_sib_r,
    ag_right, ag_left, ag_sib, ag_r, sib_r, part_s, part_r, go_s, left_r, right_r,
):
    own_rows, width = tok.shape[1], tok.shape[2]
    hidden_units = w_gate.shape[2]
    half = own_rows // HALVES
    piece = half // PIECES
    tile = width // PIECES
    count = chips * CORES
    slots = 2 * chips
    me = lax.axis_index("expert")
    p = me // CORES
    q = lax.rem(me, CORES)
    sib = p * CORES + 1 - q
    right, left = me + CORES, me - CORES
    has_right, has_left = p < chips - 1, p > 0

    def send(src, dst, send_sem, recv_sem, device):
        return pltpu.make_async_remote_copy(
            src_ref=src, dst_ref=dst, send_sem=send_sem, recv_sem=recv_sem,
            device_id={"expert": device}, device_id_type=MESH,
        )

    def gather_copy(s, c, send_sem, recv_sem, device):
        block = x.at[CORES * s + q, pl.ds(pl.multiple_of(c * piece, piece), piece)]
        return send(block, block, send_sem.at[s], recv_sem.at[s, c], device)

    def scale_copy(s, send_sem, recv_sem, device):
        block = scales.at[CORES * s + q]
        return send(block, block, send_sem.at[s], recv_sem.at[s], device)

    sides = (
        (p, has_right, right, ag_right, sc_right, from_left, left_r),
        (chips - 1 - p, has_left, left, ag_left, sc_left, from_right, right_r),
    )

    loads = [
        pltpu.make_async_copy(ids_in, expert_ids, own_sem.at[0]),
        pltpu.make_async_copy(index_in, gate_index, own_sem.at[4]),
        pltpu.make_async_copy(table_in, gate_table, own_sem.at[5]),
        pltpu.make_async_copy(spill_in, spill, own_sem.at[6]),
        pltpu.make_async_copy(w_gate.at[0], w_in.at[:, pl.ds(0, hidden_units)], own_sem.at[1]),
        pltpu.make_async_copy(w_up.at[0], w_in.at[:, pl.ds(hidden_units, hidden_units)], own_sem.at[2]),
        pltpu.make_async_copy(w_down.at[0], w_out, own_sem.at[3]),
    ]

    def own_rows_load(c):
        rows = pl.ds(pl.multiple_of(c * piece, piece), piece)
        return pltpu.make_async_copy(tok.at[0, rows], x.at[me, rows], tok_sem.at[c])

    for c in range(HALVES * PIECES):
        own_rows_load(c).start()
    for load in loads:
        load.start()
    barrier = pltpu.get_barrier_semaphore()

    def greet(device):
        pl.semaphore_signal(barrier, inc=1, device_id={"expert": device}, device_id_type=MESH)

    greet(sib)
    pl.when(has_right)(lambda: greet(right))
    pl.when(has_left)(lambda: greet(left))
    pl.semaphore_wait(barrier, 1 + has_right.astype(jnp.int32) + has_left.astype(jnp.int32))

    def first_sends(c, carry):
        own_rows_load(c).wait()
        for _, there, device, ag, *_ in sides:
            pl.when(there)(lambda: gather_copy(p, c, ag, ag_r, device).start())
        return carry

    def sib_sends(c, carry):
        pl.when(c >= PIECES)(lambda: own_rows_load(c).wait())
        gather_copy(p, c, ag_sib, sib_r, sib).start()
        return carry

    lax.fori_loop(0, PIECES, first_sends, 0)
    lax.fori_loop(0, HALVES * PIECES, sib_sends, 0)
    for load in loads[:-3]:
        load.wait()
    scales[me] = token_scales(expert_ids, gate_index, gate_table, spill, own_rows, count)
    for _, there, device, _, sc, *_ in sides:
        pl.when(there)(lambda: scale_copy(p, sc, sc_r, device).start())
    scale_copy(p, sc_sib, sc_sib_r, sib).start()

    tall = CORES * half
    wide = width // OUT_TILES
    in_tile = 2 * hidden_units // IN_TILES

    def block_rows(h):
        return pl.ds(pl.multiple_of(h * half, half), half)

    def enter(s, h):
        @pl.when((s == p) & (h == 0))
        def _():
            loads[-3].wait()
            loads[-2].wait()

        def arrived(t, carry):
            block = x.at[CORES * s + 1 - q, pl.ds(pl.multiple_of((h * PIECES + t) * piece, piece), piece)]
            send(block, block, ag_sib.at[s], sib_r.at[s, h * PIECES + t], sib).wait_recv()
            return carry

        lax.fori_loop(0, PIECES, arrived, 0)

        def one(t, carry):
            cols = pl.ds(pl.multiple_of(t * in_tile, 128), in_tile)
            tokens = x[pl.ds(CORES * s, CORES), block_rows(h)].reshape(tall, width)
            both[:, cols] = jnp.dot(tokens, w_in[:, cols], preferred_element_type=jnp.float32)
            return carry

        lax.fori_loop(0, IN_TILES, one, 0)

    def near_copy(s, h, t):
        return send(
            part.at[CORES * s + 1 - q, h, t], near.at[s, h, t],
            part_s.at[s], part_r.at[s, h * PIECES + t], sib,
        )

    def leave(s, h):
        @pl.when((s == p) & (h == 0))
        def _():
            loads[-1].wait()

        @pl.when(h == 0)
        def _():
            block = scales.at[CORES * s + 1 - q]
            send(block, block, sc_sib.at[s], sc_sib_r.at[s], sib).wait_recv()
            for core in range(CORES):
                row = scales[CORES * s + core, pl.ds(me, 1), :]
                cols_of[s, core] = jnp.transpose(jnp.broadcast_to(row, (own_rows, own_rows)))

        for core in range(CORES):
            part_rows = pl.ds(core * half, half)
            col = cols_of[s, core, block_rows(h), :][:, :1]
            gate = both[part_rows, pl.ds(0, hidden_units)]
            up = both[part_rows, pl.ds(hidden_units, hidden_units)]
            hid[part_rows, :] = (gate / (1.0 + jnp.exp(-gate)) * up * col).astype(hid.dtype)

        def one(g, carry):
            cols = pl.ds(pl.multiple_of(g * wide, 128), wide)
            made = jnp.dot(hid[...], w_out[:, cols], preferred_element_type=jnp.float32)
            made = made.astype(part.dtype).reshape(CORES, half, wide)
            for j in range(PIECES // OUT_TILES):
                t = g * (PIECES // OUT_TILES) + j
                part[pl.ds(CORES * s, CORES), h, t] = made[:, :, j * tile : (j + 1) * tile]
                near_copy(s, h, t).start()
            return carry

        lax.fori_loop(0, OUT_TILES, one, 0)

    def pair_sum(s, h, t):
        return part[CORES * s + q, h, t].astype(jnp.float32) + near[s, h, t].astype(jnp.float32)

    def came_wait(came, came_sem, s, h, t):
        block = came.at[s, h, t]
        send(block, block, go_s.at[s], came_sem.at[s, h * PIECES + t], sib).wait_recv()

    def gathers(at, side, place, there, device, ag, sc, came, came_sem):
        k, t = at // PIECES, lax.rem(at, PIECES)
        h = (k > place).astype(jnp.int32)
        origin = jnp.where(k > place, k - place - 1, place - k)
        s = origin if side == 0 else chips - 1 - origin
        active = (k > 0) & (k <= 2 * place + 1)
        c = h * PIECES + t

        @pl.when(active & (s != p))
        def _():
            gather_copy(s, c, ag, ag_r, sib).wait_recv()
            gather_copy(s, c, ag_sib, sib_r, sib).start()

            @pl.when(c == 0)
            def _():
                scale_copy(s, sc, sc_r, sib).wait_recv()
                scale_copy(s, sc_sib, sc_sib_r, sib).start()
                pl.when(there)(lambda: scale_copy(s, sc, sc_r, device).start())

        pl.when(active & there)(lambda: gather_copy(s, c, ag, ag_r, device).start())

    def sums(at, side, place, there, device, ag, sc, came, came_sem):
        k, t = at // PIECES, lax.rem(at, PIECES)
        i = k - (2 * place + 2)
        n = chips - 1 - place
        h = (i >= n).astype(jnp.int32)
        target = place + 1 + jnp.where(i >= n, 2 * n - 1 - i, i)
        s = target if side == 0 else chips - 1 - target

        @pl.when((i >= 0) & (k < slots))
        def _():
            near_copy(s, h, t).wait_recv()

            @pl.when(place == 0)
            def _():
                going[s, h, t] = pair_sum(s, h, t).astype(going.dtype)

            @pl.when(place > 0)
            def _():
                came_wait(came, came_sem, s, h, t)
                summed = pair_sum(s, h, t) + came[s, h, t].astype(jnp.float32)
                going[s, h, t] = summed.astype(going.dtype)

            send(
                going.at[s, h, t], came.at[s, h, t],
                go_s.at[s], came_sem.at[s, h * PIECES + t], device,
            ).start()

    def unit(k, second):
        mirror = (p >= chips - p) == second
        place = jnp.where(mirror, chips - 1 - p, p)
        origin = jnp.where(k > place, k - place - 1, place - k)
        own = k == 0
        s = jnp.where(own, p, jnp.where(mirror, chips - 1 - origin, origin))
        h = jnp.where(own, second.astype(jnp.int32), (k > place).astype(jnp.int32))
        return own | (k <= 2 * place), s, h

    def drain(s, carry):
        mine = x.at[CORES * s + q]
        send(mine, mine, ag_sib.at[s], ag_r.at[s, 0], sib).wait_send()
        scale_copy(s, sc_sib, sc_sib_r, sib).wait_send()
        for there, ahead, ag, sc in ((has_right, s <= p, ag_right, sc_right), (has_left, s >= p, ag_left, sc_left)):
            @pl.when(there & ahead)
            def _():
                send(mine, mine, ag.at[s], ag_r.at[s, 0], sib).wait_send()
                scale_copy(s, sc, sc_r, sib).wait_send()

        given = part.at[CORES * s + 1 - q]
        send(given, given, part_s.at[s], ag_r.at[s, 0], sib).wait_send()
        return carry

    def period(m, carry):
        at = m + LEAD
        for side, args in enumerate(sides):
            @pl.when(at < slots * PIECES)
            def _():
                gathers(at, side, *args)

        since = m - (PIECES - 1 - LEAD)
        k, phase = since // PIECES, lax.rem(since, PIECES)
        active, s, h = unit(k, phase >= PIECES // 2)
        step = lax.rem(phase, PIECES // 2)
        active &= (since >= 0) & (k < slots - 1)
        pl.when(active & (step == 0))(lambda: enter(s, h))
        pl.when(active & (step == 1))(lambda: leave(s, h))
        for side, args in enumerate(sides):
            sums(at, side, *args)

        last = m - ((slots - HALVES) * PIECES + PIECES - LEAD)
        h_last, t_last = last // PIECES, lax.rem(last, PIECES)

        @pl.when(last == PIECES)
        def _():
            lax.fori_loop(0, chips, drain, 0)

        @pl.when(last >= 0)
        def _():
            near_copy(p, h_last, t_last).wait_recv()
            total[...] = pair_sum(p, h_last, t_last)
            for there, came, came_sem in (
                (has_left, from_left, left_r), (has_right, from_right, right_r)
            ):
                @pl.when(there)
                def _():
                    came_wait(came, came_sem, p, h_last, t_last)
                    total[...] += came[p, h_last, t_last].astype(jnp.float32)

            cols = pl.ds(pl.multiple_of(t_last * tile, 128), tile)
            out[0, block_rows(h_last), cols] = total[...].astype(out.dtype)

        return carry

    lax.fori_loop(0, slots * PIECES + PIECES - LEAD, period, 0)

    def drain_sums(s, carry):
        @pl.when(s != p)
        def _():
            block = going.at[s]
            send(block, block, go_s.at[s], ag_r.at[s, 0], sib).wait_send()

        return carry

    lax.fori_loop(0, chips, drain_sums, 0)


def scratch_of(chips, own_rows, width, hidden_units, experts_all, dtype, routing):
    count = chips * CORES
    half = own_rows // HALVES
    tile = width // PIECES
    tiles = (HALVES, PIECES, half, tile)
    sums = pltpu.VMEM((chips, *tiles), dtype)
    dma = pltpu.SemaphoreType.DMA
    line = dma((chips,))
    pieces = dma((chips, HALVES * PIECES))
    return [
        *[pltpu.VMEM(value.shape, value.dtype) for value in routing],
        pltpu.VMEM((count, own_rows, width), dtype),
        pltpu.VMEM((width, 2 * hidden_units), dtype),
        pltpu.VMEM((hidden_units, width), dtype),
        pltpu.VMEM((count, experts_all, own_rows), jnp.float32),
        pltpu.VMEM((chips, CORES, own_rows, own_rows), jnp.float32),
        pltpu.VMEM((CORES * half, 2 * hidden_units), jnp.float32),
        pltpu.VMEM((CORES * half, hidden_units), dtype),
        pltpu.VMEM((count, *tiles), dtype),
        sums, sums, sums, sums,
        pltpu.VMEM((half, tile), jnp.float32),
        dma((HALVES * PIECES,)),
        dma((7,)),
        line, line, line, line, line,
        line, line, line, pieces, pieces, line, pieces, line, pieces, pieces,
    ]


def line_plan(tokens, w_gate, w_up, w_down, expert_ids, gate_index, gate_table, spill):
    experts_all = lax.axis_size("expert")
    own_rows, width = tokens.shape[1:]
    chips = experts_all // CORES
    anywhere = pl.BlockSpec(memory_space=pl.ANY)
    vmem = pl.BlockSpec(memory_space=pltpu.VMEM)
    routing = (
        jnp.swapaxes(expert_ids, 1, 2), jnp.swapaxes(gate_index, 1, 2), gate_table[None], spill
    )
    return pl.pallas_call(
        functools.partial(line_kernel, chips),
        out_shape=pltpu.VMEM(tokens.shape, tokens.dtype),
        in_specs=[anywhere] * 8,
        out_specs=vmem,
        scratch_shapes=scratch_of(
            chips, own_rows, width, w_gate.shape[2], experts_all, tokens.dtype, routing
        ),
        compiler_params=pltpu.CompilerParams(
            collective_id=0, has_side_effects=True, vmem_limit_bytes=62914560
        ),
    )(
        tokens, w_gate, w_up, w_down, *routing
    )


def local(tokens, w_gate, w_up, w_down, *routing):
    own_rows, width = tokens.shape[1:]
    experts_all = lax.axis_size("expert")
    held = w_gate.size + w_up.size + w_down.size + 4 * experts_all * own_rows * width
    fits = held * tokens.dtype.itemsize <= 56 * 2**20
    cut = own_rows % (HALVES * PIECES * 8) == 0 and width % (PIECES * 128) == 0
    line = w_gate.shape[0] == 1 and experts_all % CORES == 0 and experts_all > CORES
    if fits and cut and line:
        return line_plan(tokens, w_gate, w_up, w_down, *routing)
    return exchange_plan(tokens, w_gate, w_up, w_down, *routing)


def solution(mesh):
    in_specs = (
        P("expert", "dp", None),
        P("expert", None, None),
        P("expert", None, None),
        P("expert", None, None),
        P("expert", None, None),
        P("expert", None, None),
        P(),
        P("expert", None),
    )
    out_specs = P("expert", "dp", None)
    return jax.shard_map(local, mesh=mesh, in_specs=in_specs, out_specs=out_specs, check_vma=False)
```

```python
import functools
import jax
import jax.numpy as jnp
from jax import lax
from jax.experimental import pallas as pl
from jax.experimental.pallas import tpu as pltpu
from jax.sharding import PartitionSpec as P


def exchange_plan(tokens, w_gate, w_up, w_down, expert_ids, gate_index, gate_table, spill):
    dp_count = lax.axis_size("dp")
    expert_count = lax.axis_size("expert")
    local_experts = w_gate.shape[0]
    experts_all = local_experts * expert_count
    own_rows = tokens.shape[1]
    model_width = tokens.shape[2]
    column_tokens = spill.shape[1]
    top_count = expert_ids.shape[2]
    capacity = 3 * own_rows * top_count // (2 * experts_all)
    spill_room = own_rows // 4
    dp_index = lax.axis_index("dp")
    senders = spill[0]
    flat_ids = expert_ids[0].reshape(-1)
    level_count = gate_table.shape[0]
    matches = gate_index[0][:, :, None] == jnp.arange(level_count, dtype=jnp.int32)
    picked = jnp.sum(jnp.where(matches, gate_table, 0.0), axis=2)
    weight = picked / jnp.sum(picked, axis=1, keepdims=True)
    pair_sender = jnp.repeat(senders, top_count)
    is_mine = pair_sender == dp_index
    onehot = (
        (flat_ids[:, None] == jnp.arange(experts_all, dtype=jnp.int32)) & is_mine[:, None]
    ).astype(jnp.int32)
    slot_rank = jnp.sum((jnp.cumsum(onehot, axis=0) - onehot) * onehot, axis=1)
    is_kept = is_mine & (slot_rank < capacity)
    empty_slot = experts_all * capacity
    slot_index = jnp.where(is_kept, flat_ids * capacity + slot_rank, empty_slot)
    pair_token = jnp.arange(column_tokens * top_count, dtype=jnp.int32) // top_count
    zero_row = jnp.zeros((1, model_width), tokens.dtype)
    token_ids = jnp.arange(column_tokens, dtype=jnp.int32)
    home_dev = token_ids // own_rows
    local_token = token_ids - home_dev * own_rows
    is_moved = senders != home_dev
    route_key = home_dev * dp_count + senders
    route_hot = (route_key[:, None] == jnp.arange(dp_count * dp_count, dtype=jnp.int32)).astype(
        jnp.int32
    )
    spill_rank = jnp.sum((jnp.cumsum(route_hot, axis=0) - route_hot) * route_hot, axis=1)
    incoming = is_moved & (senders == dp_index)
    spill_slots = dp_count * spill_room
    outgoing = is_moved & (home_dev == dp_index)
    send_target = jnp.where(outgoing, senders * spill_room + spill_rank, spill_slots)
    send_source = (
        jnp.full((spill_slots,), own_rows, jnp.int32).at[send_target].set(local_token, mode="drop")
    )
    own_padded = jnp.concatenate([tokens[0], zero_row], axis=0)
    outgoing_rows = own_padded[send_source].reshape(dp_count, spill_room, model_width)
    arrived = lax.all_to_all(outgoing_rows, "dp", split_axis=0, concat_axis=0, tiled=True)
    source_rows = jnp.concatenate(
        [tokens[0], arrived.reshape(spill_slots, model_width), zero_row], axis=0
    )
    token_row = jnp.where(
        home_dev == dp_index,
        local_token,
        jnp.where(incoming, own_rows + home_dev * spill_room + spill_rank, own_rows + spill_slots),
    )
    dispatch_source = (
        jnp.full((empty_slot,), source_rows.shape[0] - 1, jnp.int32)
        .at[slot_index]
        .set(token_row[pair_token], mode="drop")
    )
    outbound = source_rows[dispatch_source].reshape(
        expert_count, local_experts, capacity, model_width
    )
    block = lax.all_to_all(outbound, "expert", split_axis=0, concat_axis=0, tiled=True)
    gate_part = jnp.einsum("aecd,edf->aecf", block, w_gate, preferred_element_type=jnp.float32)
    up_part = jnp.einsum("aecd,edf->aecf", block, w_up, preferred_element_type=jnp.float32)
    hidden = (jax.nn.silu(gate_part) * up_part).astype(jnp.bfloat16)
    expert_out = jnp.einsum(
        "aecf,efd->aecd", hidden, w_down, preferred_element_type=jnp.float32
    ).astype(jnp.bfloat16)
    returned = lax.all_to_all(expert_out, "expert", split_axis=0, concat_axis=0, tiled=True)
    results = jnp.concatenate([returned.reshape(empty_slot, model_width), zero_row], axis=0)
    slot_grid = jnp.concatenate(
        [
            slot_index.reshape(column_tokens, top_count),
            jnp.full((1, top_count), empty_slot, jnp.int32),
        ],
        axis=0,
    )
    kept_scale = jnp.where(is_kept.reshape(column_tokens, top_count), weight, 0.0)
    scale_grid = jnp.concatenate([kept_scale, jnp.zeros((1, top_count), jnp.float32)], axis=0)

    def combine(chosen):
        chosen_slots = slot_grid[chosen]
        chosen_scale = scale_grid[chosen]
        summed = jnp.zeros((chosen.shape[0], model_width), jnp.float32)
        for member in range(top_count):
            summed = summed + chosen_scale[:, member : member + 1] * results[
                chosen_slots[:, member]
            ].astype(jnp.float32)
        return summed

    own_ids = dp_index * own_rows + jnp.arange(own_rows, dtype=jnp.int32)
    own_part = combine(own_ids)
    arrived_target = jnp.where(incoming, home_dev * spill_room + spill_rank, spill_slots)
    arrived_ids = (
        jnp.full((spill_slots,), column_tokens, jnp.int32)
        .at[arrived_target]
        .set(token_ids, mode="drop")
    )
    arrived_part = combine(arrived_ids).reshape(dp_count, spill_room, model_width)
    returned_part = lax.all_to_all(
        arrived_part.astype(jnp.bfloat16), "dp", split_axis=0, concat_axis=0, tiled=True
    ).astype(arrived_part.dtype)
    back_rows = jnp.concatenate(
        [returned_part.reshape(spill_slots, model_width), jnp.zeros((1, model_width), jnp.float32)],
        axis=0,
    )
    back_pick = jnp.where(
        is_moved[own_ids], senders[own_ids] * spill_room + spill_rank[own_ids], spill_slots
    )
    mixed = own_part + back_rows[back_pick]
    return mixed.astype(jnp.bfloat16)[None]


CORES = 2
HALVES = 2
PIECES = 4
LEAD = PIECES // 2
IN_TILES = 1
OUT_TILES = 2
MESH = pl.DeviceIdType.MESH


def token_scales(expert_ids, gate_index, gate_table, spill, own_rows, experts_all):
    top_count, column_tokens = expert_ids.shape[1:]
    capacity = 3 * own_rows * top_count // (2 * experts_all)
    first = pl.multiple_of(lax.axis_index("dp") * own_rows, own_rows)
    own = pl.ds(first, own_rows)
    experts = lax.broadcasted_iota(jnp.int32, (experts_all, column_tokens), 0)
    chosen = jnp.zeros((experts_all, column_tokens), jnp.float32)
    for k in range(top_count):
        chosen += jnp.where(expert_ids[0, k : k + 1, :] == experts, 1.0, 0.0)
    own_row = spill[:, own].astype(jnp.float32)
    own_senders = jnp.transpose(jnp.broadcast_to(own_row, (own_rows, own_rows)))[:, :1]
    shape = (own_rows, column_tokens)
    before = lax.broadcasted_iota(jnp.int32, shape, 1) < first + lax.broadcasted_iota(
        jnp.int32, shape, 0
    )
    earlier = before & (spill[...].astype(jnp.float32) == own_senders)
    rank = lax.dot_general(
        chosen.astype(jnp.bfloat16),
        jnp.where(earlier, 1.0, 0.0).astype(jnp.bfloat16),
        (((1,), (1,)), ((), ())),
        preferred_element_type=jnp.float32,
    )
    level_count = gate_table.shape[1]
    levels = lax.broadcasted_iota(jnp.int32, (level_count, own_rows), 0)
    table = jnp.transpose(jnp.broadcast_to(gate_table[...], (own_rows, level_count)))
    picked = [
        jnp.sum(
            jnp.where(gate_index[0, k : k + 1, own] == levels, table, 0.0), axis=0, keepdims=True
        )
        for k in range(top_count)
    ]
    norm = functools.reduce(jnp.add, picked)
    own_experts = lax.broadcasted_iota(jnp.int32, (experts_all, own_rows), 0)
    scale = jnp.zeros((experts_all, own_rows), jnp.float32)
    for k in range(top_count):
        scale += jnp.where(expert_ids[0, k : k + 1, own] == own_experts, picked[k] / norm, 0.0)
    return jnp.where(rank < capacity, scale, 0.0)


def line_kernel(
    chips, tok, w_gate, w_up, w_down, ids_in, index_in, table_in, spill_in, out,
    expert_ids, gate_index, gate_table, spill, x, w_in, w_out, scales, cols_of, both, hid, part, near, from_left, from_right, going, total,
    tok_sem, own_sem, to_right, to_left, to_sib, sc_right, sc_left, sc_sib, sc_r, sc_sib_r,
    ag_r, sib_r, part_r, sum_r,
):
    own_rows, width = tok.shape[1], tok.shape[2]
    hidden_units = w_gate.shape[2]
    half = own_rows // HALVES
    piece = half // PIECES
    tile = width // PIECES
    count = chips * CORES
    slots = 2 * chips
    me = lax.axis_index("expert")
    p = me // CORES
    q = lax.rem(me, CORES)
    sib = p * CORES + 1 - q
    right, left = me + CORES, me - CORES
    has_right, has_left = p < chips - 1, p > 0

    def send(src, dst, send_sem, recv_sem, device):
        return pltpu.make_async_remote_copy(
            src_ref=src, dst_ref=dst, send_sem=send_sem, recv_sem=recv_sem,
            device_id={"expert": device}, device_id_type=MESH,
        )

    def rows_of(s, core, c):
        return x.at[CORES * s + core, pl.ds(pl.multiple_of(c * piece, piece), piece)]

    def gather_copy(s, c, send_sem, to, device):
        block = rows_of(s, q, c)
        return send(block, block, send_sem, ag_r.at[jnp.where(s > to, s - 1, s), c], device)

    def sib_copy(s, c):
        block = rows_of(s, q, c)
        return send(block, block, to_sib, sib_r.at[s, c // PIECES], sib)

    def scale_copy(s, send_sem, recv_sem, device):
        block = scales.at[CORES * s + q]
        return send(block, block, send_sem, recv_sem.at[s], device)

    sides = (
        (p, has_right, right, p + 1, to_right, sc_right, from_left),
        (chips - 1 - p, has_left, left, p - 1, to_left, sc_left, from_right),
    )

    loads = [
        pltpu.make_async_copy(ids_in, expert_ids, own_sem.at[0]),
        pltpu.make_async_copy(index_in, gate_index, own_sem.at[1]),
        pltpu.make_async_copy(table_in, gate_table, own_sem.at[2]),
        pltpu.make_async_copy(spill_in, spill, own_sem.at[3]),
        pltpu.make_async_copy(w_gate.at[0], w_in.at[:, pl.ds(0, hidden_units)], own_sem.at[4]),
        pltpu.make_async_copy(w_up.at[0], w_in.at[:, pl.ds(hidden_units, hidden_units)], own_sem.at[4]),
        pltpu.make_async_copy(w_down.at[0], w_out, own_sem.at[5]),
    ]

    def own_rows_load(h):
        rows = pl.ds(h * half, half)
        return pltpu.make_async_copy(tok.at[0, rows], x.at[me, rows], tok_sem.at[h])

    for h in range(HALVES):
        own_rows_load(h).start()
    for load in loads[:-3]:
        load.start()
    barrier = pltpu.get_barrier_semaphore()

    def greet(device):
        pl.semaphore_signal(barrier, inc=1, device_id={"expert": device}, device_id_type=MESH)

    greet(sib)
    pl.when(has_right)(lambda: greet(right))
    pl.when(has_left)(lambda: greet(left))
    pl.semaphore_wait(barrier, 1 + has_right.astype(jnp.int32) + has_left.astype(jnp.int32))

    def first_sends(c, carry):
        for _, there, device, to, gone, *_ in sides:
            pl.when(there)(lambda: gather_copy(p, c, gone, to, device).start())
        return carry

    def sib_sends(c, carry):
        sib_copy(p, c).start()
        return carry

    own_rows_load(0).wait()
    lax.fori_loop(0, PIECES, first_sends, 0)
    own_rows_load(1).wait()
    lax.fori_loop(0, HALVES * PIECES, sib_sends, 0)
    for load in loads[-3:]:
        load.start()
    for load in loads[:-3]:
        load.wait()
    scales[me] = token_scales(expert_ids, gate_index, gate_table, spill, own_rows, count)
    for _, there, device, _, _, sc, _ in sides:
        pl.when(there)(lambda: scale_copy(p, sc, sc_r, device).start())
    scale_copy(p, sc_sib, sc_sib_r, sib).start()

    tall = CORES * half
    wide = width // OUT_TILES
    in_tile = 2 * hidden_units // IN_TILES

    def block_rows(h):
        return pl.ds(pl.multiple_of(h * half, half), half)

    def enter(s, h):
        @pl.when((s == p) & (h == 0))
        def _():
            pltpu.make_async_copy(w_in, w_in, own_sem.at[4]).wait()

        block = x.at[CORES * s + 1 - q, block_rows(h)]
        send(block, block, to_sib, sib_r.at[s, h], sib).wait_recv()

        def one(t, carry):
            cols = pl.ds(pl.multiple_of(t * in_tile, 128), in_tile)
            tokens = x[pl.ds(CORES * s, CORES), block_rows(h)].reshape(tall, width)
            both[:, cols] = jnp.dot(tokens, w_in[:, cols], preferred_element_type=jnp.float32)
            return carry

        lax.fori_loop(0, IN_TILES, one, 0)

    def near_copy(s, h, t):
        return send(
            part.at[CORES * s + 1 - q, h, t], near.at[s, h, t],
            to_sib, part_r.at[s, h], sib,
        )

    def near_wait(s, h):
        block = near.at[s, h]
        send(block, block, to_sib, part_r.at[s, h], sib).wait_recv()

    def leave(s, h):
        @pl.when((s == p) & (h == 0))
        def _():
            loads[-1].wait()

        @pl.when(h == 0)
        def _():
            block = scales.at[CORES * s + 1 - q]
            send(block, block, sc_sib, sc_sib_r.at[s], sib).wait_recv()
            for core in range(CORES):
                row = scales[CORES * s + core, pl.ds(me, 1), :]
                cols_of[s, core] = jnp.transpose(jnp.broadcast_to(row, (own_rows, own_rows)))

        for core in range(CORES):
            part_rows = pl.ds(core * half, half)
            col = cols_of[s, core, block_rows(h), :][:, :1]
            gate = both[part_rows, pl.ds(0, hidden_units)]
            up = both[part_rows, pl.ds(hidden_units, hidden_units)]
            hid[part_rows, :] = (gate / (1.0 + jnp.exp(-gate)) * up * col).astype(hid.dtype)

        def one(g, carry):
            cols = pl.ds(pl.multiple_of(g * wide, 128), wide)
            made = jnp.dot(hid[...], w_out[:, cols], preferred_element_type=jnp.float32)
            made = made.astype(part.dtype).reshape(CORES, half, wide)
            for j in range(PIECES // OUT_TILES):
                t = g * (PIECES // OUT_TILES) + j
                part[pl.ds(CORES * s, CORES), h, t] = made[:, :, j * tile : (j + 1) * tile]
                near_copy(s, h, t).start()
            return carry

        lax.fori_loop(0, OUT_TILES, one, 0)

    def pair_sum(s, h, t):
        return part[CORES * s + q, h, t].astype(jnp.float32) + near[s, h, t].astype(jnp.float32)

    def sum_sem(side, s, h, t):
        return sum_r.at[s + 1 if side == 0 else s, h * PIECES + t]

    def came_wait(side, came, s, h, t):
        block = came.at[s, h, t]
        send(block, block, to_sib, sum_sem(side, s, h, t), sib).wait_recv()

    def gathers(at, side, place, there, device, to, gone, sc, came):
        k, t = at // PIECES, lax.rem(at, PIECES)
        h = (k > place).astype(jnp.int32)
        origin = jnp.where(k > place, k - place - 1, place - k)
        s = origin if side == 0 else chips - 1 - origin
        active = (k > 0) & (k <= 2 * place + 1)
        c = h * PIECES + t

        @pl.when(active & (s != p))
        def _():
            gather_copy(s, c, gone, p, sib).wait_recv()
            sib_copy(s, c).start()

            @pl.when(c == 0)
            def _():
                scale_copy(s, sc, sc_r, sib).wait_recv()
                scale_copy(s, sc_sib, sc_sib_r, sib).start()
                pl.when(there)(lambda: scale_copy(s, sc, sc_r, device).start())

        pl.when(active & there)(lambda: gather_copy(s, c, gone, to, device).start())

    def sums(at, side, place, there, device, to, gone, sc, came):
        k, t = at // PIECES, lax.rem(at, PIECES)
        i = k - (2 * place + 2)
        n = chips - 1 - place
        h = (i >= n).astype(jnp.int32)
        target = place + 1 + jnp.where(i >= n, 2 * n - 1 - i, i)
        s = target if side == 0 else chips - 1 - target

        @pl.when((i >= 0) & (k < slots))
        def _():
            pl.when(t == 0)(lambda: near_wait(s, h))

            @pl.when(place == 0)
            def _():
                going[s, h, t] = pair_sum(s, h, t).astype(going.dtype)

            @pl.when(place > 0)
            def _():
                came_wait(side, came, s, h, t)
                summed = pair_sum(s, h, t) + came[s, h, t].astype(jnp.float32)
                going[s, h, t] = summed.astype(going.dtype)

            send(
                going.at[s, h, t], came.at[s, h, t], gone, sum_sem(side, s, h, t), device
            ).start()

    def unit(k, second):
        mirror = (p >= chips - p) == second
        place = jnp.where(mirror, chips - 1 - p, p)
        origin = jnp.where(k > place, k - place - 1, place - k)
        own = k == 0
        s = jnp.where(own, p, jnp.where(mirror, chips - 1 - origin, origin))
        h = jnp.where(own, second.astype(jnp.int32), (k > place).astype(jnp.int32))
        return own | (k <= 2 * place), s, h

    def period(m, carry):
        at = m + LEAD
        for side, args in enumerate(sides):
            @pl.when(at < slots * PIECES)
            def _():
                gathers(at, side, *args)

        since = m - (PIECES - 1 - LEAD)
        k, phase = since // PIECES, lax.rem(since, PIECES)
        active, s, h = unit(k, phase >= PIECES // 2)
        step = lax.rem(phase, PIECES // 2)
        active &= (since >= 0) & (k < slots - 1)
        pl.when(active & (step == 0))(lambda: enter(s, h))
        pl.when(active & (step == 1))(lambda: leave(s, h))
        for side, args in enumerate(sides):
            sums(at, side, *args)

        last = m - ((slots - HALVES) * PIECES + PIECES - LEAD)
        h_last, t_last = last // PIECES, lax.rem(last, PIECES)

        @pl.when(last >= 0)
        def _():
            pl.when(t_last == 0)(lambda: near_wait(p, h_last))
            total[...] = pair_sum(p, h_last, t_last)
            for side, (place, *_, came) in enumerate(sides):
                @pl.when(place > 0)
                def _():
                    came_wait(side, came, p, h_last, t_last)
                    total[...] += came[p, h_last, t_last].astype(jnp.float32)

            cols = pl.ds(pl.multiple_of(t_last * tile, 128), tile)
            out[0, block_rows(h_last), cols] = total[...].astype(out.dtype)

        return carry

    lax.fori_loop(0, slots * PIECES + PIECES - LEAD, period, 0)

    for place, there, _, _, gone, sc, _ in sides:
        @pl.when(there)
        def _():
            block = x.at[pl.ds(0, chips)]
            send(block, block, gone, sib_r.at[0, 0], sib).wait_send()

        for k in range(chips):
            @pl.when(there & (place == k))
            def _():
                block = scales.at[pl.ds(0, k + 1)]
                send(block, block, sc, sib_r.at[0, 0], sib).wait_send()

    block = scales.at[pl.ds(0, chips)]
    send(block, block, sc_sib, sib_r.at[0, 0], sib).wait_send()
    send(x, x, to_sib, sib_r.at[0, 0], sib).wait_send()


def scratch_of(chips, own_rows, width, hidden_units, experts_all, dtype, routing):
    count = chips * CORES
    half = own_rows // HALVES
    tile = width // PIECES
    tiles = (HALVES, PIECES, half, tile)
    sums = pltpu.VMEM((chips, *tiles), dtype)
    dma = pltpu.SemaphoreType.DMA
    return [
        *[pltpu.VMEM(value.shape, value.dtype) for value in routing],
        pltpu.VMEM((count, own_rows, width), dtype),
        pltpu.VMEM((width, 2 * hidden_units), dtype),
        pltpu.VMEM((hidden_units, width), dtype),
        pltpu.VMEM((count, experts_all, own_rows), jnp.float32),
        pltpu.VMEM((chips, CORES, own_rows, own_rows), jnp.float32),
        pltpu.VMEM((CORES * half, 2 * hidden_units), jnp.float32),
        pltpu.VMEM((CORES * half, hidden_units), dtype),
        pltpu.VMEM((count, *tiles), dtype),
        sums, sums, sums, sums,
        pltpu.VMEM((half, tile), jnp.float32),
        dma((HALVES,)),
        dma((6,)),
        dma, dma, dma, dma, dma, dma,
        dma((chips,)),
        dma((chips,)),
        dma((chips - 1, HALVES * PIECES)),
        dma((chips, HALVES)),
        dma((chips, HALVES)),
        dma((chips + 1, HALVES * PIECES)),
    ]


def line_plan(tokens, w_gate, w_up, w_down, expert_ids, gate_index, gate_table, spill):
    experts_all = lax.axis_size("expert")
    own_rows, width = tokens.shape[1:]
    chips = experts_all // CORES
    anywhere = pl.BlockSpec(memory_space=pl.ANY)
    vmem = pl.BlockSpec(memory_space=pltpu.VMEM)
    routing = (
        jnp.swapaxes(expert_ids, 1, 2), jnp.swapaxes(gate_index, 1, 2), gate_table[None], spill
    )
    return pl.pallas_call(
        functools.partial(line_kernel, chips),
        out_shape=pltpu.VMEM(tokens.shape, tokens.dtype),
        in_specs=[anywhere] * 8,
        out_specs=vmem,
        scratch_shapes=scratch_of(
            chips, own_rows, width, w_gate.shape[2], experts_all, tokens.dtype, routing
        ),
        compiler_params=pltpu.CompilerParams(
            collective_id=0, has_side_effects=True, vmem_limit_bytes=62914560
        ),
    )(
        tokens, w_gate, w_up, w_down, *routing
    )


def local(tokens, w_gate, w_up, w_down, *routing):
    own_rows, width = tokens.shape[1:]
    experts_all = lax.axis_size("expert")
    held = w_gate.size + w_up.size + w_down.size + 4 * experts_all * own_rows * width
    fits = held * tokens.dtype.itemsize <= 56 * 2**20
    cut = own_rows % (HALVES * PIECES * 8) == 0 and width % (PIECES * 128) == 0
    line = w_gate.shape[0] == 1 and experts_all % CORES == 0 and experts_all > CORES
    if fits and cut and line:
        return line_plan(tokens, w_gate, w_up, w_down, *routing)
    return exchange_plan(tokens, w_gate, w_up, w_down, *routing)


def solution(mesh):
    in_specs = (
        P("expert", "dp", None),
        P("expert", None, None),
        P("expert", None, None),
        P("expert", None, None),
        P("expert", None, None),
        P("expert", None, None),
        P(),
        P("expert", None),
    )
    out_specs = P("expert", "dp", None)
    return jax.shard_map(local, mesh=mesh, in_specs=in_specs, out_specs=out_specs, check_vma=False)
```

```python
import functools
import jax
import jax.numpy as jnp
from jax import lax
from jax.experimental import pallas as pl
from jax.experimental.pallas import tpu as pltpu
from jax.sharding import PartitionSpec as P


def exchange_plan(tokens, w_gate, w_up, w_down, expert_ids, gate_index, gate_table, spill):
    dp_count = lax.axis_size("dp")
    expert_count = lax.axis_size("expert")
    local_experts = w_gate.shape[0]
    experts_all = local_experts * expert_count
    own_rows = tokens.shape[1]
    model_width = tokens.shape[2]
    column_tokens = spill.shape[1]
    top_count = expert_ids.shape[2]
    capacity = 3 * own_rows * top_count // (2 * experts_all)
    spill_room = own_rows // 4
    dp_index = lax.axis_index("dp")
    senders = spill[0]
    flat_ids = expert_ids[0].reshape(-1)
    level_count = gate_table.shape[0]
    matches = gate_index[0][:, :, None] == jnp.arange(level_count, dtype=jnp.int32)
    picked = jnp.sum(jnp.where(matches, gate_table, 0.0), axis=2)
    weight = picked / jnp.sum(picked, axis=1, keepdims=True)
    pair_sender = jnp.repeat(senders, top_count)
    is_mine = pair_sender == dp_index
    onehot = (
        (flat_ids[:, None] == jnp.arange(experts_all, dtype=jnp.int32)) & is_mine[:, None]
    ).astype(jnp.int32)
    slot_rank = jnp.sum((jnp.cumsum(onehot, axis=0) - onehot) * onehot, axis=1)
    is_kept = is_mine & (slot_rank < capacity)
    empty_slot = experts_all * capacity
    slot_index = jnp.where(is_kept, flat_ids * capacity + slot_rank, empty_slot)
    pair_token = jnp.arange(column_tokens * top_count, dtype=jnp.int32) // top_count
    zero_row = jnp.zeros((1, model_width), tokens.dtype)
    token_ids = jnp.arange(column_tokens, dtype=jnp.int32)
    home_dev = token_ids // own_rows
    local_token = token_ids - home_dev * own_rows
    is_moved = senders != home_dev
    route_key = home_dev * dp_count + senders
    route_hot = (route_key[:, None] == jnp.arange(dp_count * dp_count, dtype=jnp.int32)).astype(
        jnp.int32
    )
    spill_rank = jnp.sum((jnp.cumsum(route_hot, axis=0) - route_hot) * route_hot, axis=1)
    incoming = is_moved & (senders == dp_index)
    spill_slots = dp_count * spill_room
    outgoing = is_moved & (home_dev == dp_index)
    send_target = jnp.where(outgoing, senders * spill_room + spill_rank, spill_slots)
    send_source = (
        jnp.full((spill_slots,), own_rows, jnp.int32).at[send_target].set(local_token, mode="drop")
    )
    own_padded = jnp.concatenate([tokens[0], zero_row], axis=0)
    outgoing_rows = own_padded[send_source].reshape(dp_count, spill_room, model_width)
    arrived = lax.all_to_all(outgoing_rows, "dp", split_axis=0, concat_axis=0, tiled=True)
    source_rows = jnp.concatenate(
        [tokens[0], arrived.reshape(spill_slots, model_width), zero_row], axis=0
    )
    token_row = jnp.where(
        home_dev == dp_index,
        local_token,
        jnp.where(incoming, own_rows + home_dev * spill_room + spill_rank, own_rows + spill_slots),
    )
    dispatch_source = (
        jnp.full((empty_slot,), source_rows.shape[0] - 1, jnp.int32)
        .at[slot_index]
        .set(token_row[pair_token], mode="drop")
    )
    outbound = source_rows[dispatch_source].reshape(
        expert_count, local_experts, capacity, model_width
    )
    block = lax.all_to_all(outbound, "expert", split_axis=0, concat_axis=0, tiled=True)
    gate_part = jnp.einsum("aecd,edf->aecf", block, w_gate, preferred_element_type=jnp.float32)
    up_part = jnp.einsum("aecd,edf->aecf", block, w_up, preferred_element_type=jnp.float32)
    hidden = (jax.nn.silu(gate_part) * up_part).astype(jnp.bfloat16)
    expert_out = jnp.einsum(
        "aecf,efd->aecd", hidden, w_down, preferred_element_type=jnp.float32
    ).astype(jnp.bfloat16)
    returned = lax.all_to_all(expert_out, "expert", split_axis=0, concat_axis=0, tiled=True)
    results = jnp.concatenate([returned.reshape(empty_slot, model_width), zero_row], axis=0)
    slot_grid = jnp.concatenate(
        [
            slot_index.reshape(column_tokens, top_count),
            jnp.full((1, top_count), empty_slot, jnp.int32),
        ],
        axis=0,
    )
    kept_scale = jnp.where(is_kept.reshape(column_tokens, top_count), weight, 0.0)
    scale_grid = jnp.concatenate([kept_scale, jnp.zeros((1, top_count), jnp.float32)], axis=0)

    def combine(chosen):
        chosen_slots = slot_grid[chosen]
        chosen_scale = scale_grid[chosen]
        summed = jnp.zeros((chosen.shape[0], model_width), jnp.float32)
        for member in range(top_count):
            summed = summed + chosen_scale[:, member : member + 1] * results[
                chosen_slots[:, member]
            ].astype(jnp.float32)
        return summed

    own_ids = dp_index * own_rows + jnp.arange(own_rows, dtype=jnp.int32)
    own_part = combine(own_ids)
    arrived_target = jnp.where(incoming, home_dev * spill_room + spill_rank, spill_slots)
    arrived_ids = (
        jnp.full((spill_slots,), column_tokens, jnp.int32)
        .at[arrived_target]
        .set(token_ids, mode="drop")
    )
    arrived_part = combine(arrived_ids).reshape(dp_count, spill_room, model_width)
    returned_part = lax.all_to_all(
        arrived_part.astype(jnp.bfloat16), "dp", split_axis=0, concat_axis=0, tiled=True
    ).astype(arrived_part.dtype)
    back_rows = jnp.concatenate(
        [returned_part.reshape(spill_slots, model_width), jnp.zeros((1, model_width), jnp.float32)],
        axis=0,
    )
    back_pick = jnp.where(
        is_moved[own_ids], senders[own_ids] * spill_room + spill_rank[own_ids], spill_slots
    )
    mixed = own_part + back_rows[back_pick]
    return mixed.astype(jnp.bfloat16)[None]


CORES = 2
HALVES = 2
PIECES = 4
PAIR = 2
LEAD = PIECES // 2
IN_TILES = 1
OUT_TILES = 2
MESH = pl.DeviceIdType.MESH


def token_scales(expert_ids, gate_index, gate_table, spill, own_rows, experts_all):
    top_count, column_tokens = expert_ids.shape[1:]
    capacity = 3 * own_rows * top_count // (2 * experts_all)
    first = pl.multiple_of(lax.axis_index("dp") * own_rows, own_rows)
    own = pl.ds(first, own_rows)
    experts = lax.broadcasted_iota(jnp.int32, (experts_all, column_tokens), 0)
    chosen = jnp.zeros((experts_all, column_tokens), jnp.float32)
    for k in range(top_count):
        chosen += jnp.where(expert_ids[0, k : k + 1, :] == experts, 1.0, 0.0)
    own_row = spill[:, own].astype(jnp.float32)
    own_senders = jnp.transpose(jnp.broadcast_to(own_row, (own_rows, own_rows)))[:, :1]
    shape = (own_rows, column_tokens)
    before = lax.broadcasted_iota(jnp.int32, shape, 1) < first + lax.broadcasted_iota(
        jnp.int32, shape, 0
    )
    earlier = before & (spill[...].astype(jnp.float32) == own_senders)
    rank = lax.dot_general(
        chosen.astype(jnp.bfloat16),
        jnp.where(earlier, 1.0, 0.0).astype(jnp.bfloat16),
        (((1,), (1,)), ((), ())),
        preferred_element_type=jnp.float32,
    )
    level_count = gate_table.shape[1]
    levels = lax.broadcasted_iota(jnp.int32, (level_count, own_rows), 0)
    table = jnp.transpose(jnp.broadcast_to(gate_table[...], (own_rows, level_count)))
    picked = [
        jnp.sum(
            jnp.where(gate_index[0, k : k + 1, own] == levels, table, 0.0), axis=0, keepdims=True
        )
        for k in range(top_count)
    ]
    norm = functools.reduce(jnp.add, picked)
    own_experts = lax.broadcasted_iota(jnp.int32, (experts_all, own_rows), 0)
    scale = jnp.zeros((experts_all, own_rows), jnp.float32)
    for k in range(top_count):
        scale += jnp.where(expert_ids[0, k : k + 1, own] == own_experts, picked[k] / norm, 0.0)
    return jnp.where(rank < capacity, scale, 0.0)


def line_kernel(
    chips, tok, w_gate, w_up, w_down, ids_in, index_in, table_in, spill_in, out,
    expert_ids, gate_index, gate_table, spill, x, w_in, w_out, scales, cols_of, both, hid, part, near, from_left, from_right, going,
    tok_sem, own_sem, to_right, to_left, to_sib, sc_right, sc_left, sc_sib, sc_r, sc_sib_r,
    ag_r, sib_r, part_r, sum_r,
):
    own_rows, width = tok.shape[1], tok.shape[2]
    hidden_units = w_gate.shape[2]
    half = own_rows // HALVES
    piece = half // PIECES
    tile = width // PIECES
    count = chips * CORES
    slots = 2 * chips
    me = lax.axis_index("expert")
    p = me // CORES
    q = lax.rem(me, CORES)
    sib = p * CORES + 1 - q
    right, left = me + CORES, me - CORES
    has_right, has_left = p < chips - 1, p > 0

    def send(src, dst, send_sem, recv_sem, device):
        return pltpu.make_async_remote_copy(
            src_ref=src, dst_ref=dst, send_sem=send_sem, recv_sem=recv_sem,
            device_id={"expert": device}, device_id_type=MESH,
        )

    def rows_of(s, core, c):
        return x.at[CORES * s + core, pl.ds(pl.multiple_of(c * piece, piece), piece)]

    def gather_copy(s, c, send_sem, to, device):
        block = rows_of(s, q, c)
        return send(block, block, send_sem, ag_r.at[jnp.where(s > to, s - 1, s), c // PAIR], device)

    def pair_wait(s, pair):
        rows = pl.ds(pl.multiple_of(pair * PAIR * piece, PAIR * piece), PAIR * piece)
        block = x.at[CORES * s + q, rows]
        send(block, block, to_sib, ag_r.at[jnp.where(s > p, s - 1, s), pair], sib).wait_recv()

    def sib_copy(s, c):
        block = rows_of(s, q, c)
        return send(block, block, to_sib, sib_r.at[s, c // PIECES], sib)

    def scale_copy(s, send_sem, recv_sem, device):
        block = scales.at[CORES * s + q]
        return send(block, block, send_sem, recv_sem.at[s], device)

    sides = (
        (p, has_right, right, p + 1, to_right, sc_right, from_left),
        (chips - 1 - p, has_left, left, p - 1, to_left, sc_left, from_right),
    )

    barrier = pltpu.get_barrier_semaphore()

    def greet(device):
        pl.semaphore_signal(barrier, inc=1, device_id={"expert": device}, device_id_type=MESH)

    greet(sib)
    pl.when(has_right)(lambda: greet(right))
    pl.when(has_left)(lambda: greet(left))
    loads = [
        pltpu.make_async_copy(ids_in, expert_ids, own_sem.at[0]),
        pltpu.make_async_copy(index_in, gate_index, own_sem.at[1]),
        pltpu.make_async_copy(table_in, gate_table, own_sem.at[2]),
        pltpu.make_async_copy(spill_in, spill, own_sem.at[3]),
        pltpu.make_async_copy(w_gate.at[0], w_in.at[:, pl.ds(0, hidden_units)], own_sem.at[4]),
        pltpu.make_async_copy(w_up.at[0], w_in.at[:, pl.ds(hidden_units, hidden_units)], own_sem.at[4]),
        pltpu.make_async_copy(w_down.at[0], w_out, own_sem.at[5]),
    ]

    def own_rows_load(h):
        rows = pl.ds(h * half, half)
        return pltpu.make_async_copy(tok.at[0, rows], x.at[me, rows], tok_sem.at[h])

    for h in range(HALVES):
        own_rows_load(h).start()
    for load in loads[:-3]:
        load.start()
    pl.semaphore_wait(barrier, 1 + has_right.astype(jnp.int32) + has_left.astype(jnp.int32))

    def first_sends(c, carry):
        for _, there, device, to, gone, *_ in sides:
            pl.when(there)(lambda: gather_copy(p, c, gone, to, device).start())
        return carry

    def sib_sends(c, carry):
        sib_copy(p, c).start()
        return carry

    own_rows_load(0).wait()
    lax.fori_loop(0, PIECES, first_sends, 0)
    own_rows_load(1).wait()
    lax.fori_loop(0, HALVES * PIECES, sib_sends, 0)
    for load in loads[-3:]:
        load.start()
    for load in loads[:-3]:
        load.wait()
    scales[me] = token_scales(expert_ids, gate_index, gate_table, spill, own_rows, count)
    for _, there, device, _, _, sc, _ in sides:
        pl.when(there)(lambda: scale_copy(p, sc, sc_r, device).start())
    scale_copy(p, sc_sib, sc_sib_r, sib).start()

    tall = CORES * half
    wide = width // OUT_TILES
    in_tile = 2 * hidden_units // IN_TILES

    def block_rows(h):
        return pl.ds(pl.multiple_of(h * half, half), half)

    def enter(s, h):
        @pl.when((s == p) & (h == 0))
        def _():
            pltpu.make_async_copy(w_in, w_in, own_sem.at[4]).wait()

        block = x.at[CORES * s + 1 - q, block_rows(h)]
        send(block, block, to_sib, sib_r.at[s, h], sib).wait_recv()

        def one(t, carry):
            cols = pl.ds(pl.multiple_of(t * in_tile, 128), in_tile)
            tokens = x[pl.ds(CORES * s, CORES), block_rows(h)].reshape(tall, width)
            both[:, cols] = jnp.dot(tokens, w_in[:, cols], preferred_element_type=jnp.float32)
            return carry

        lax.fori_loop(0, IN_TILES, one, 0)

    def near_copy(s, h, t):
        return send(
            part.at[CORES * s + 1 - q, h, t], near.at[s, h, t],
            to_sib, part_r.at[s, h], sib,
        )

    def near_wait(s, h):
        block = near.at[s, h]
        send(block, block, to_sib, part_r.at[s, h], sib).wait_recv()

    def leave(s, h):
        @pl.when((s == p) & (h == 0))
        def _():
            loads[-1].wait()

        @pl.when(h == 0)
        def _():
            block = scales.at[CORES * s + 1 - q]
            send(block, block, sc_sib, sc_sib_r.at[s], sib).wait_recv()
            for core in range(CORES):
                row = scales[CORES * s + core, pl.ds(me, 1), :]
                cols_of[s, core] = jnp.transpose(jnp.broadcast_to(row, (own_rows, own_rows)))

        for core in range(CORES):
            part_rows = pl.ds(core * half, half)
            col = cols_of[s, core, block_rows(h), :][:, :1]
            gate = both[part_rows, pl.ds(0, hidden_units)]
            up = both[part_rows, pl.ds(hidden_units, hidden_units)]
            hid[part_rows, :] = (gate / (1.0 + jnp.exp(-gate)) * up * col).astype(hid.dtype)

        def one(g, carry):
            cols = pl.ds(pl.multiple_of(g * wide, 128), wide)
            made = jnp.dot(hid[...], w_out[:, cols], preferred_element_type=jnp.float32)
            made = made.astype(part.dtype).reshape(CORES, half, wide)
            for j in range(PIECES // OUT_TILES):
                t = g * (PIECES // OUT_TILES) + j
                part[pl.ds(CORES * s, CORES), h, t] = made[:, :, j * tile : (j + 1) * tile]
                near_copy(s, h, t).start()
            return carry

        lax.fori_loop(0, OUT_TILES, one, 0)

    def pair_sum(s, h, t):
        return part[CORES * s + q, h, t].astype(jnp.float32) + near[s, h, t].astype(jnp.float32)

    def sum_sem(side, s, h, t):
        return sum_r.at[s + 1 if side == 0 else s, h * (PIECES // PAIR) + t // PAIR]

    def came_wait(side, came, s, h, t):
        @pl.when(lax.rem(t, PAIR) == 0)
        def _():
            block = came.at[s, h, pl.ds(t // PAIR * PAIR, PAIR)]
            send(block, block, to_sib, sum_sem(side, s, h, t), sib).wait_recv()

    def gathers(at, side, place, there, device, to, gone, sc, came):
        k, t = at // PIECES, lax.rem(at, PIECES)
        h = (k > place).astype(jnp.int32)
        origin = jnp.where(k > place, k - place - 1, place - k)
        s = origin if side == 0 else chips - 1 - origin
        active = (k > 0) & (k <= 2 * place + 1)
        c = h * PIECES + t

        @pl.when(active & (s != p))
        def _():
            pl.when(lax.rem(t, PAIR) == 0)(lambda: pair_wait(s, c // PAIR))
            sib_copy(s, c).start()

            @pl.when(c == 0)
            def _():
                scale_copy(s, sc, sc_r, sib).wait_recv()
                scale_copy(s, sc_sib, sc_sib_r, sib).start()
                pl.when(there)(lambda: scale_copy(s, sc, sc_r, device).start())

        pl.when(active & there)(lambda: gather_copy(s, c, gone, to, device).start())

    def sums(at, side, place, there, device, to, gone, sc, came):
        k, t = at // PIECES, lax.rem(at, PIECES)
        i = k - (2 * place + 2)
        n = chips - 1 - place
        h = (i >= n).astype(jnp.int32)
        target = place + 1 + jnp.where(i >= n, 2 * n - 1 - i, i)
        s = target if side == 0 else chips - 1 - target

        @pl.when((i >= 0) & (k < slots))
        def _():
            pl.when(t == 0)(lambda: near_wait(s, h))

            @pl.when(place == 0)
            def _():
                going[s, h, t] = pair_sum(s, h, t).astype(going.dtype)

            @pl.when(place > 0)
            def _():
                came_wait(side, came, s, h, t)
                summed = pair_sum(s, h, t) + came[s, h, t].astype(jnp.float32)
                going[s, h, t] = summed.astype(going.dtype)

            send(
                going.at[s, h, t], came.at[s, h, t], gone, sum_sem(side, s, h, t), device
            ).start()

    def unit(k, second):
        mirror = (p >= chips - p) == second
        place = jnp.where(mirror, chips - 1 - p, p)
        origin = jnp.where(k > place, k - place - 1, place - k)
        own = k == 0
        s = jnp.where(own, p, jnp.where(mirror, chips - 1 - origin, origin))
        h = jnp.where(own, second.astype(jnp.int32), (k > place).astype(jnp.int32))
        return own | (k <= 2 * place), s, h

    def drain():
        for place, there, _, _, _, sc, _ in sides:
            for k in range(chips):
                @pl.when(there & (place == k))
                def _():
                    block = scales.at[pl.ds(0, k + 1)]
                    send(block, block, sc, sib_r.at[0, 0], sib).wait_send()

        block = scales.at[pl.ds(0, chips)]
        send(block, block, sc_sib, sib_r.at[0, 0], sib).wait_send()
        send(x, x, to_sib, sib_r.at[0, 0], sib).wait_send()

    def period(m, carry):
        at = m + LEAD
        for side, args in enumerate(sides):
            @pl.when(at < slots * PIECES)
            def _():
                gathers(at, side, *args)

        since = m - (PIECES - 1 - LEAD)
        k, phase = since // PIECES, lax.rem(since, PIECES)
        active, s, h = unit(k, phase >= PIECES // 2)
        step = lax.rem(phase, PIECES // 2)
        active &= (since >= 0) & (k < slots - 1)
        pl.when(active & (step == 0))(lambda: enter(s, h))
        pl.when(active & (step == 1))(lambda: leave(s, h))
        for side, args in enumerate(sides):
            sums(at, side, *args)

        last = m - ((slots - HALVES) * PIECES + PIECES - LEAD)
        h_last, t_last = last // PIECES, lax.rem(last, PIECES)

        pl.when(last == PIECES)(drain)

        @pl.when(last >= 0)
        def _():
            pl.when(t_last == 0)(lambda: near_wait(p, h_last))
            cols = pl.ds(pl.multiple_of(t_last * tile, 128), tile)
            for side, (place, *_, came) in enumerate(sides):
                pl.when(place > 0)(lambda: came_wait(side, came, p, h_last, t_last))

            def finish(*arrived):
                total = pair_sum(p, h_last, t_last)
                for came in arrived:
                    total += came[p, h_last, t_last].astype(jnp.float32)
                out[0, block_rows(h_last), cols] = total.astype(out.dtype)

            pl.when(has_left & has_right)(lambda: finish(from_left, from_right))
            pl.when(jnp.logical_not(has_left))(lambda: finish(from_right))
            pl.when(jnp.logical_not(has_right))(lambda: finish(from_left))

        return carry

    lax.fori_loop(0, slots * PIECES + PIECES - LEAD, period, 0)

    for _, there, _, _, gone, *_ in sides:
        @pl.when(there)
        def _():
            block = x.at[pl.ds(0, chips)]
            send(block, block, gone, sib_r.at[0, 0], sib).wait_send()


def scratch_of(chips, own_rows, width, hidden_units, experts_all, dtype, routing):
    count = chips * CORES
    half = own_rows // HALVES
    tile = width // PIECES
    tiles = (HALVES, PIECES, half, tile)
    sums = pltpu.VMEM((chips, *tiles), dtype)
    dma = pltpu.SemaphoreType.DMA
    return [
        *[pltpu.VMEM(value.shape, value.dtype) for value in routing],
        pltpu.VMEM((count, own_rows, width), dtype),
        pltpu.VMEM((width, 2 * hidden_units), dtype),
        pltpu.VMEM((hidden_units, width), dtype),
        pltpu.VMEM((count, experts_all, own_rows), jnp.float32),
        pltpu.VMEM((chips, CORES, own_rows, own_rows), jnp.float32),
        pltpu.VMEM((CORES * half, 2 * hidden_units), jnp.float32),
        pltpu.VMEM((CORES * half, hidden_units), dtype),
        pltpu.VMEM((count, *tiles), dtype),
        sums, sums, sums, sums,
        dma((HALVES,)),
        dma((6,)),
        dma, dma, dma, dma, dma, dma,
        dma((chips,)),
        dma((chips,)),
        dma((chips - 1, HALVES * PIECES // PAIR)),
        dma((chips, HALVES)),
        dma((chips, HALVES)),
        dma((chips + 1, HALVES * PIECES // PAIR)),
    ]


def line_plan(tokens, w_gate, w_up, w_down, expert_ids, gate_index, gate_table, spill):
    experts_all = lax.axis_size("expert")
    own_rows, width = tokens.shape[1:]
    chips = experts_all // CORES
    anywhere = pl.BlockSpec(memory_space=pl.ANY)
    vmem = pl.BlockSpec(memory_space=pltpu.VMEM)
    routing = (
        jnp.swapaxes(expert_ids, 1, 2), jnp.swapaxes(gate_index, 1, 2), gate_table[None], spill
    )
    return pl.pallas_call(
        functools.partial(line_kernel, chips),
        out_shape=pltpu.VMEM(tokens.shape, tokens.dtype),
        in_specs=[anywhere] * 8,
        out_specs=vmem,
        scratch_shapes=scratch_of(
            chips, own_rows, width, w_gate.shape[2], experts_all, tokens.dtype, routing
        ),
        compiler_params=pltpu.CompilerParams(
            collective_id=0, has_side_effects=True, vmem_limit_bytes=62914560
        ),
    )(
        tokens, w_gate, w_up, w_down, *routing
    )


def local(tokens, w_gate, w_up, w_down, *routing):
    own_rows, width = tokens.shape[1:]
    experts_all = lax.axis_size("expert")
    held = w_gate.size + w_up.size + w_down.size + 4 * experts_all * own_rows * width
    fits = held * tokens.dtype.itemsize <= 56 * 2**20
    cut = own_rows % (HALVES * PIECES * 8) == 0 and width % (PIECES * 128) == 0
    line = w_gate.shape[0] == 1 and experts_all % CORES == 0 and experts_all > CORES
    if fits and cut and line:
        return line_plan(tokens, w_gate, w_up, w_down, *routing)
    return exchange_plan(tokens, w_gate, w_up, w_down, *routing)


def solution(mesh):
    in_specs = (
        P("expert", "dp", None),
        P("expert", None, None),
        P("expert", None, None),
        P("expert", None, None),
        P("expert", None, None),
        P("expert", None, None),
        P(),
        P("expert", None),
    )
    out_specs = P("expert", "dp", None)
    return jax.shard_map(local, mesh=mesh, in_specs=in_specs, out_specs=out_specs, check_vma=False)
```
